256 devices in a mesh: param: 128 (over z, x, y), sensor: 2 (over core).
Axes of the slice: x: 4, y: 4, z: 8, core: 2. Of those that a mesh axis runs over, the one named last changes fastest.
Arguments:
- data: float32 [16, 512, 420], P(None, ('sensor', 'param')), may hold values from -6 to 6
- spectra: float32 [2, 512, 512, 421], P(None, 'sensor', 'param'), may hold values from -2 to 2
Outputs:
- gradient: float32 [16, 512, 420], P(None, 'param')
- rms: float32 [16], replicated
The draws below stay inside these ranges and needn't reach their ends.
All inputs are finite; a program needn't handle non-finite values.
Results may differ from the reference program's by a relative error of at most 0.0003.
Values sent between devices are 32-bit elements; how exact they have to be, the bound alone decides.
A program may use at most 128 MiB of HBM per device.

```python
import math
import jax
import jax.numpy as jnp
from jax import lax

SENSORS = 512
NT = 420
NF = 421
P_DEV = 4
NRHS = 16
PARAMS = 512
N_PARAM = 128


def draw_spectra(key, part):
    first = jax.random.fold_in(key, 0)
    shape = (2, SENSORS, PARAMS, NF)
    ramp = 1.0 + jnp.arange(PARAMS, dtype=jnp.float32) / max(PARAMS - 1, 1)
    base = jnp.clip(jax.random.normal(first, shape, jnp.float32), -6.0, 6.0)
    base = base * ramp[None, None, :, None]
    return jnp.clip(base / math.sqrt(SENSORS), -2.0, 2.0)


def shard_levels(rng, dims, cuts, smallest, largest):
    gain = 1.0
    for dim, blocks in cuts:
        heights = jax.random.uniform(jax.random.fold_in(jax.random.fold_in(rng, 6), dim), (blocks,), jnp.float32, smallest / len(cuts), largest / len(cuts))
        gain = gain * jnp.repeat(jnp.exp(heights), dims[dim] // blocks).reshape((-1,) + (1,) * (len(dims) - 1 - dim))
    return gain


def gaussian(rng, shape, scale, limit, shards=(), kind=jnp.bfloat16):
    values = jax.random.normal(rng, shape, jnp.float32) * scale
    if len(shards) > 0:
        values = shard_levels(rng, shape, shards, -0.22, 0.18) * values
    return jnp.clip(values, min=-limit, max=limit).astype(kind)


def setup_inputs(seed: int = 0) -> dict:
    seeds = jax.random.split(jax.random.key(seed), 3)
    data = gaussian(seeds[0], (NRHS, SENSORS, NT), 1.0, 6.0, ((1, 256),), jnp.float32)
    spectra = draw_spectra(jax.random.fold_in(seeds[2], 71), 0)
    return dict(data=data, spectra=spectra)


def reference(data, spectra):
    data_hat = jnp.fft.rfft(data, n=2 * NT, axis=-1)
    real_part = jnp.real(data_hat).astype(jnp.float32)
    imag_part = jnp.imag(data_hat).astype(jnp.float32)

    def one_block(index):
        start = (index * P_DEV).astype(jnp.int32)
        kernel = lax.dynamic_slice_in_dim(spectra, start, P_DEV, 2)
        kernel_re = kernel[0]
        kernel_im = kernel[1]
        hi = lax.Precision.HIGHEST
        out_re = jnp.einsum('spf,rsf->rpf', kernel_re, real_part, precision=hi) + jnp.einsum('spf,rsf->rpf', kernel_im, imag_part, precision=hi)
        out_im = jnp.einsum('spf,rsf->rpf', kernel_re, imag_part, precision=hi) - jnp.einsum('spf,rsf->rpf', kernel_im, real_part, precision=hi)
        return (out_re, out_im)
    blocks_re, blocks_im = lax.map(one_block, jnp.arange(N_PARAM, dtype=jnp.int32))
    whole_re = jnp.transpose(blocks_re, (1, 0, 2, 3)).reshape(data.shape[0], PARAMS, NF)
    whole_im = jnp.transpose(blocks_im, (1, 0, 2, 3)).reshape(data.shape[0], PARAMS, NF)
    field = jnp.fft.irfft(whole_re + 1j * whole_im, n=2 * NT, axis=-1)[..., :NT].astype(jnp.float32)
    rms = jnp.sqrt(lax.optimization_barrier(jnp.mean(field * field, axis=(1, 2))) + 1e-06)
    return (field / rms[:, None, None], rms)
```

```python
import functools
import math
import random

import jax
import jax.numpy as jnp
import numpy as np
from jax import lax
from jax.experimental import pallas as pl
from jax.experimental.pallas import tpu as pltpu
from jax.sharding import Mesh
from jax.sharding import PartitionSpec as P

PARAM = ("param_0", "param_1", "param_2")
SENSOR_PARAM = ("sensor", "param_0", "param_1", "param_2")
MESH = pl.DeviceIdType.MESH
F32 = jnp.float32
BF16 = jnp.bfloat16
TORUS = (8, 4, 4)
DIRS = ((0, 1, 0), (0, -1, 0), (0, 0, 1), (0, 0, -1), (1, 0, 0), (-1, 0, 0))
EXTRA = (2, 0, 0)
ROWS = 112
LANES = 128
PIECE = 45
REST = 37
SETUP_STEPS = 4
VMEM_LIMIT = 66_800_000


def moved(offset, step):
    return tuple((a + b) % n for a, b, n in zip(offset, step, TORUS))


def attempt(seed):
    rng = random.Random(seed)
    got = {(0, 0, 0): 0, EXTRA: 2}
    steps = []
    number = (math.prod(TORUS) - 2) // 6
    for k in range(1, number + 1):
        for lag in (3, 2, 1):
            cand = []
            for d in range(6):
                edges = []
                for p, s in got.items():
                    c = moved(p, DIRS[d])
                    if c in got or (s > 0 and s > k - min(lag, max(1, k - 1))):
                        continue
                    edges.append((s, rng.random(), p, c))
                cand.append(sorted(edges))
            used = {}

            def augment(d, seen):
                for s, _, p, c in cand[d]:
                    if c in seen:
                        continue
                    seen.add(c)
                    if c not in used or augment(used[c][0], seen):
                        used[c] = (d, p)
                        return True
                return False

            count = sum(augment(d, set()) for d in sorted(range(6), key=lambda d: len(cand[d])))
            if count == 6:
                break
        else:
            return None
        for c, (d, p) in used.items():
            got[c] = k
        steps.append(sorted((d, p, c) for c, (d, p) in used.items()))
    lags = [k - got[p] for k, step in enumerate(steps, 1) for d, p, c in step if got[p] > 0 and k > 3]
    return (sum(10 ** (3 - lag) for lag in lags if lag < 3), steps)


def make_schedule():
    best = None
    for seed in range(150):
        found = attempt(seed)
        if found and (best is None or found[0] < best[0]):
            best = found
    return best[1]


def spectral_tables(steps):
    half = steps // 2
    t = np.arange(steps)[:, None]
    even = 2 * np.arange(half + 1)[None, :]
    odd = 2 * np.arange(half)[None, :] + 1
    turn = math.pi / steps
    even_re = np.cos(turn * (t * even % (2 * steps)))
    even_im = -np.sin(turn * (t * even % (2 * steps)))
    even_im[:, 0] = np.arange(steps) == 0
    even_im[:, half] = 0.0
    odd_re = np.cos(turn * (t * odd % (2 * steps)))
    odd_im = -np.sin(turn * (t * odd % (2 * steps)))
    forward = np.zeros((512, 512))
    forward[:steps, : half + 1] = even_re
    forward[:steps, 256 : 256 + half + 1] = even_im
    weight = np.full((half + 1,), 2.0 / steps)
    weight[0] = weight[half] = 1.0 / steps
    across = np.zeros((2, 256, 256))
    across[0, : half + 1, :half] = weight[:, None] * (even_re.T @ odd_im)
    across[1, : half + 1, :half] = weight[:, None] * (even_im.T @ odd_re)
    across[1, 0, :half] = 1.0
    gains = np.zeros((8, 512))
    gains[0, : half + 1] = weight / 2
    gains[0, 256 : 256 + half] = 1.0 / steps
    gains[1] = gains[0]
    gains[1, 0] = 0.0
    return (forward, across, gains)


def high_low(array):
    array = array.astype(np.float32)
    high = array.astype(jnp.bfloat16)
    low = (array - high.astype(np.float32)).astype(jnp.bfloat16)
    return (high, low)


def split(value):
    high = value.astype(BF16)
    return (high, (value - high.astype(F32)).astype(BF16))


def times(value, high, low, transposed=False):
    dims = (((1,), (1 if transposed else 0,)), ((), ()))
    dot = functools.partial(lax.dot_general, dimension_numbers=dims, preferred_element_type=F32)
    upper, lower = split(value)
    return dot(upper, high) + dot(lower, high) + dot(upper, low)


def kernel(
    steps,
    data_ref,
    k_ref,
    fh_ref,
    fl_ref,
    ah_ref,
    al_ref,
    gain_ref,
    field_ref,
    rms_ref,
    gat,
    xv,
    xs,
    kraw,
    kt,
    fh,
    fl,
    ah,
    al,
    gain,
    eb,
    do,
    acc,
    part,
    other,
    red1,
    red2,
    srow,
    send_sem,
    recv_sem,
    load_sem,
    pair_sem,
    r1_send,
    r1_recv,
    r2_send,
    r2_recv,
):
    vectors, own, length = data_ref.shape
    me = tuple(lax.axis_index(name) for name in PARAM)
    core = lax.axis_index("sensor")

    def device(offset):
        return {
            name: lax.rem(pos + (o % n), n) for name, pos, o, n in zip(PARAM, me, offset, TORUS)
        }

    partner = {"sensor": 1 - core}
    barrier = pltpu.get_barrier_semaphore()
    for offset in DIRS + (tuple(-o for o in EXTRA),):
        pl.semaphore_signal(barrier, inc=1, device_id=device(offset), device_id_type=MESH)
    pl.semaphore_signal(barrier, inc=1, device_id=partner, device_id_type=MESH)

    rows_k = k_ref.shape[1]
    loads = [
        pltpu.make_async_copy(data_ref, xv, load_sem.at[0]),
        pltpu.make_async_copy(fh_ref, fh, load_sem.at[1]),
        pltpu.make_async_copy(fl_ref, fl, load_sem.at[2]),
        pltpu.make_async_copy(k_ref, kraw.at[:, pl.ds(0, rows_k), :], load_sem.at[3]),
        pltpu.make_async_copy(ah_ref, ah, load_sem.at[4]),
        pltpu.make_async_copy(al_ref, al, load_sem.at[5]),
        pltpu.make_async_copy(gain_ref, gain, load_sem.at[6]),
    ]
    for load in loads:
        load.start()

    slot_of = {(0, 0, 0): 0, EXTRA: 1}
    for k, step in enumerate(steps):
        for i, (d, p, c) in enumerate(step):
            slot_of[c] = 2 + 6 * k + i
    step_of = {c: k for k, step in enumerate(steps, 1) for d, p, c in step}
    step_of[(0, 0, 0)] = 0
    step_of[EXTRA] = 2
    pending = {}
    for k, step in enumerate(steps):
        for d, p, c in step:
            pending.setdefault(step_of[p], []).append((d, p, c))

    def copy(source, target, offset):
        return pltpu.make_async_remote_copy(
            src_ref=gat.at[source],
            dst_ref=gat.at[target],
            send_sem=send_sem.at[target],
            recv_sem=recv_sem.at[target],
            device_id=device(offset),
            device_id_type=MESH,
        )

    def forward_after(k):
        for d, p, c in pending.get(k, ()):
            copy(slot_of[p], slot_of[c], DIRS[d]).start()

    xs[:, pl.ds(384, LANES)] = jnp.zeros((2 * vectors, LANES), F32)
    loads[0].wait()
    for r in range(vectors):
        for s in range(own):
            xs[pl.ds(s * vectors + r, 1), pl.ds(0, length)] = xv[r, pl.ds(s, 1), :]
    loads[1].wait()
    loads[2].wait()
    spec = times(xs[...], fh[...], fl[...])
    lane = lax.broadcasted_iota(jnp.int32, (32, LANES), 1)
    lane8 = lax.broadcasted_iota(jnp.int32, (8, LANES), 1)
    re_b = spec[:, 128:256]
    im_b = spec[:, 384:512]
    gat[0, pl.ds(0, 32), :] = spec[:, 0:128]
    gat[0, pl.ds(32, 32), :] = spec[:, 256:384]
    gat[0, pl.ds(64, 32), :] = re_b + pltpu.roll(
        jnp.where(lane < PIECE, im_b, 0.0), LANES - PIECE, 1
    )
    rest = jnp.where((lane >= PIECE) & (lane < PIECE + REST), im_b, 0.0)
    groups = [
        pltpu.roll(rest[8 * g : 8 * g + 8], (REST * (g % 3) - PIECE) % LANES, 1) for g in range(4)
    ]
    gat[0, pl.ds(96, 8), :] = groups[0] + groups[1] + groups[2]
    gat[0, pl.ds(104, 8), :] = groups[3]

    pl.semaphore_wait(barrier, 8)
    forward_after(0)
    copy(0, 1, EXTRA).start()

    for offset, slot in slot_of.items():
        z, x, y = (
            lax.rem(pos + n - o, n) for pos, o, n in zip(me, offset, TORUS)
        )
        srow[slot] = ((z * TORUS[1] + x) * TORUS[2] + y) * own * 8

    acc[...] = jnp.zeros(acc.shape, F32)
    for c in range(2):
        tail_rows = kraw.shape[1] - rows_k
        kraw[c, pl.ds(rows_k, tail_rows), :] = jnp.zeros((tail_rows, LANES), F32)
    loads[3].wait()
    loads[4].wait()
    loads[5].wait()
    loads[6].wait()

    def transpose_tile(ft):
        parity, half = divmod(ft, 2)
        base = (2 * half * LANES + parity) * 8

        @pl.loop(0, 8)
        def _(i):
            st = i // 4
            p = lax.rem(i, 4)
            for c in range(2):
                block = kraw[c, pl.ds(base + st * 4 + p, LANES, stride=16), :]
                turned = block.T
                if c == 1 and ft == 0:
                    first = lax.broadcasted_iota(jnp.int32, (LANES, LANES), 1) == 0
                    turned = jnp.where(first, 0.0, turned)
                kt[ft, pl.ds(st * LANES * 8 + c * 4 + p, LANES, stride=8), :] = turned

    def wait_slot(slot):
        copy(0, slot, DIRS[0]).wait_recv()

    def consume(first, count):
        number = 32 * count
        for j in range(count):
            tile2 = gat[first + j, pl.ds(64, 32), :]
            left = gat[first + j, pl.ds(96, 16), :]
            moved2 = pltpu.roll(tile2, PIECE, 1)
            for g in range(4):
                source = left[8:16] if g == 3 else left[0:8]
                back = pltpu.roll(source, (PIECE - REST * (g % 3)) % LANES, 1)
                value = jnp.where(
                    lane8 < PIECE,
                    moved2[8 * g : 8 * g + 8],
                    jnp.where(lane8 < PIECE + REST, back, 0.0),
                )
                eb[pl.ds(32 * j + 8 * g, 8), :] = value

        def tiles(row):
            return gat[pl.ds(first, count), pl.ds(row, 32), :].reshape(number, LANES)

        even_re = jnp.concatenate([tiles(0), tiles(64)], axis=1)
        do[pl.ds(0, number), pl.ds(256, 256)] = times(even_re, ah[0], al[0])
        even_im = jnp.concatenate([tiles(32), eb[pl.ds(0, number), :]], axis=1)
        do[pl.ds(0, number), pl.ds(0, 256)] = times(even_im, ah[1], al[1])

        def d_value(ft, j, s, h, imag):
            inner = s * 16 + h * 8
            if ft == 0:
                return gat[first + j, pl.ds((32 if imag else 0) + inner, 8), :]
            if ft == 1:
                if imag:
                    return eb[pl.ds(pl.multiple_of(j * 32 + inner, 8), 8), :]
                return gat[first + j, pl.ds(64 + inner, 8), :]
            return do[
                pl.ds(pl.multiple_of(j * 32 + inner, 8), 8),
                pl.ds((256 if imag else 0) + (ft - 2) * LANES, LANES),
            ]

        for ft in range(4):
            start = tuple(
                acc[c, pl.ds(p * 16 + h * 8, 8), pl.ds(ft * LANES, LANES)]
                for c in range(2)
                for p in range(4)
                for h in range(2)
            )

            def sensors(j, sums):
                sums = list(sums)
                row = srow[first + j]
                for s in range(own):
                    d_re = [d_value(ft, j, s, h, False) for h in range(2)]
                    d_im = [d_value(ft, j, s, h, True) for h in range(2)]
                    for p in range(4):
                        at = pl.multiple_of(row + s * 8, 8)
                        k_re = jnp.broadcast_to(kt[ft, pl.ds(at + p, 1), :], (8, LANES))
                        k_im = jnp.broadcast_to(kt[ft, pl.ds(at + 4 + p, 1), :], (8, LANES))
                        for h in range(2):
                            i = p * 2 + h
                            sums[i] = sums[i] + k_re * d_re[h] + k_im * d_im[h]
                            sums[8 + i] = sums[8 + i] + k_re * d_im[h] - k_im * d_re[h]
                return tuple(sums)

            final = lax.fori_loop(0, count, sensors, start)
            for i, value in enumerate(final):
                c, p, h = i // 8, i // 2 % 4, i % 2
                acc[c, pl.ds(p * 16 + h * 8, 8), pl.ds(ft * LANES, LANES)] = value

    last = len(steps)

    @pl.loop(1, last + 1)
    def _(k):
        for i in range(6):
            wait_slot(2 + 6 * (k - 1) + i)

        @pl.when(k == 2)
        def _():
            wait_slot(1)

        for number in range(1, last):
            if number in pending:

                @pl.when(k == number)
                def _():
                    forward_after(number)

        @pl.when(k <= SETUP_STEPS)
        def _():
            for ft in range(4):

                @pl.when(k == ft + 1)
                def _():
                    transpose_tile(ft)

        @pl.when(k == SETUP_STEPS)
        def _():
            consume(0, 2)

        caught = 2 * SETUP_STEPS
        low = jnp.where(k <= SETUP_STEPS, 0, jnp.where(k <= caught, 2 * (k - SETUP_STEPS) - 2, k - 1))
        high = jnp.where(k <= SETUP_STEPS, 0, jnp.where(k <= caught, 2 * (k - SETUP_STEPS), k))

        @pl.loop(low, high)
        def _(b):
            consume(2 + 6 * b, 6)

    out_re = acc[0] * gain[0:1, :]
    out_im = acc[1] * gain[1:2, :]
    s_re = out_re[:, 0:256] + times(out_im[:, 256:512], ah[0], al[0], True)
    s_im = out_im[:, 0:256] + times(out_re[:, 256:512], ah[1], al[1], True)
    total = times(s_re, fh[:, 0:256], fl[:, 0:256], True) + times(
        s_im, fh[:, 256:512], fl[:, 256:512], True
    )
    part[...] = total
    swap = pltpu.make_async_remote_copy(
        src_ref=part,
        dst_ref=other,
        send_sem=pair_sem.at[0],
        recv_sem=pair_sem.at[1],
        device_id=partner,
        device_id_type=MESH,
    )
    swap.start()
    for slot in range(1, gat.shape[0]):
        copy(0, slot, DIRS[0]).wait_send()
    swap.wait()
    field = part[...] + other[...]
    field_ref[...] = field
    square = field * field
    square = square[:, 0:128] + square[:, 128:256] + square[:, 256:384] + square[:, 384:512]
    square = square[0:16] + square[16:32] + square[32:48] + square[48:64]

    z, x, y = me
    spot = x * TORUS[2] + y
    red1[spot] = square
    sends = []
    for dx in range(TORUS[1]):
        for dy in range(TORUS[2]):
            i = dx * TORUS[2] + dy
            if i == 0:
                continue
            sends.append(
                pltpu.make_async_remote_copy(
                    src_ref=red1.at[spot],
                    dst_ref=red1.at[spot],
                    send_sem=r1_send.at[i],
                    recv_sem=r1_recv.at[i],
                    device_id=device((0, dx, dy)),
                    device_id_type=MESH,
                )
            )
    for send in sends:
        send.start()
    for send in sends:
        send.wait()
    plane = red1[0]
    for i in range(1, TORUS[1] * TORUS[2]):
        plane = plane + red1[i]
    red2[z] = plane
    sends = []
    for dz in range(1, TORUS[0]):
        sends.append(
            pltpu.make_async_remote_copy(
                src_ref=red2.at[z],
                dst_ref=red2.at[z],
                send_sem=r2_send.at[dz],
                recv_sem=r2_recv.at[dz],
                device_id=device((dz, 0, 0)),
                device_id_type=MESH,
            )
        )
    for send in sends:
        send.start()
    for send in sends:
        send.wait()
    whole = red2[0]
    for i in range(1, TORUS[0]):
        whole = whole + red2[i]
    count = 4 * math.prod(TORUS) * length
    mean = jnp.sum(whole, axis=1, keepdims=True) / count
    rms_ref[...] = jnp.broadcast_to(jnp.sqrt(mean + 1e-6), rms_ref.shape)


def body(data, spectra):
    vectors, own, length = data.shape
    freqs = length + 1
    sensors = spectra.shape[1]
    points = spectra.shape[2]
    forward, across, gains = spectral_tables(length)
    fh, fl = high_low(forward)
    ah, al = high_low(across)
    k_rows = jnp.transpose(
        spectra.reshape(2, sensors // LANES, LANES, points, freqs), (0, 4, 1, 3, 2)
    ).reshape(2, freqs * 8, LANES)
    steps = make_schedule()
    devices = math.prod(TORUS)
    vmem = pltpu.VMEM
    field, rms = pl.pallas_call(
        functools.partial(kernel, steps),
        out_shape=(
            jax.ShapeDtypeStruct((points * vectors, 512), F32),
            jax.ShapeDtypeStruct((vectors, LANES), F32),
        ),
        in_specs=[pl.BlockSpec(memory_space=pltpu.HBM)] * 7,
        out_specs=[pl.BlockSpec(memory_space=pltpu.VMEM)] * 2,
        scratch_shapes=[
            vmem((devices, ROWS, LANES), F32),
            vmem((vectors, own, length), F32),
            vmem((vectors * own, 512), F32),
            vmem((2, 4096, LANES), F32),
            vmem((4, sensors * 8, LANES), F32),
            vmem((512, 512), BF16),
            vmem((512, 512), BF16),
            vmem((2, 256, 256), BF16),
            vmem((2, 256, 256), BF16),
            vmem((8, 512), F32),
            vmem((192, LANES), F32),
            vmem((192, 512), F32),
            vmem((2, points * vectors, 512), F32),
            vmem((points * vectors, 512), F32),
            vmem((points * vectors, 512), F32),
            vmem((16, vectors, LANES), F32),
            vmem((8, vectors, LANES), F32),
            pltpu.SMEM((devices,), jnp.int32),
            pltpu.SemaphoreType.DMA((devices,)),
            pltpu.SemaphoreType.DMA((devices,)),
            pltpu.SemaphoreType.DMA((7,)),
            pltpu.SemaphoreType.DMA((2,)),
            pltpu.SemaphoreType.DMA((16,)),
            pltpu.SemaphoreType.DMA((16,)),
            pltpu.SemaphoreType.DMA((8,)),
            pltpu.SemaphoreType.DMA((8,)),
        ],
        compiler_params=pltpu.CompilerParams(
            collective_id=0, has_side_effects=True, vmem_limit_bytes=VMEM_LIMIT
        ),
        name="adjoint",
    )(data, k_rows, jnp.asarray(fh), jnp.asarray(fl), jnp.asarray(ah), jnp.asarray(al), jnp.asarray(gains, F32))
    scale = rms[:, 0]
    shaped = jnp.transpose(field.reshape(points, vectors, 512)[..., :length], (1, 0, 2))
    return (shaped / scale[:, None, None], scale)


def solution(mesh):
    split_mesh = Mesh(
        mesh.devices.reshape(*TORUS, mesh.shape["sensor"]), (*PARAM, "sensor")
    )
    placed = (P(None, SENSOR_PARAM, None), P(None, "sensor", PARAM, None))
    return jax.shard_map(
        body, mesh=split_mesh, in_specs=placed, out_specs=(P(None, PARAM, None), P()), check_vma=False
    )
```

```python
import functools
import math
import random

import jax
import jax.numpy as jnp
import numpy as np
from jax import lax
from jax.experimental import pallas as pl
from jax.experimental.pallas import tpu as pltpu
from jax.sharding import Mesh
from jax.sharding import PartitionSpec as P

PARAM = ("param_0", "param_1", "param_2")
SENSOR_PARAM = ("sensor", "param_0", "param_1", "param_2")
MESH = pl.DeviceIdType.MESH
F32 = jnp.float32
BF16 = jnp.bfloat16
TORUS = (8, 4, 4)
DIRS = ((0, 1, 0), (0, -1, 0), (0, 0, 1), (0, 0, -1), (1, 0, 0), (-1, 0, 0))
EXTRA = (1, 1, 0)
ROWS = 112
SENT = 107
LAG = 4
SEED = 80
LANES = 128
PIECE = 45
REST = 37
UNROLL = 6
VMEM_LIMIT = 66_000_000


def moved(offset, step):
    return tuple((a + b) % n for a, b, n in zip(offset, step, TORUS))


def make_schedule():
    rng = random.Random(SEED)
    got = {(0, 0, 0): 0, EXTRA: 2}
    steps = []
    number = (math.prod(TORUS) - 2) // len(DIRS)
    for k in range(1, number + 1):
        for lag in range(LAG, 0, -1):
            cand = []
            for d in range(len(DIRS)):
                edges = []
                for p, s in got.items():
                    c = moved(p, DIRS[d])
                    if c in got or (s > 0 and s > k - min(lag, max(1, k - 1))):
                        continue
                    key = 0 if k <= LAG else -sum(moved(c, e) not in got for e in DIRS)
                    edges.append((key, rng.random(), p, c))
                cand.append(sorted(edges))
            used = {}

            def augment(d, seen):
                for _, _, p, c in cand[d]:
                    if c in seen:
                        continue
                    seen.add(c)
                    if c not in used or augment(used[c][0], seen):
                        used[c] = (d, p)
                        return True
                return False

            order = sorted(range(len(DIRS)), key=lambda d: len(cand[d]))
            if sum(augment(d, set()) for d in order) == len(DIRS):
                break
        for c, (d, p) in used.items():
            got[c] = k
        steps.append(sorted((d, p, c) for c, (d, p) in used.items()))
    assert len(got) == math.prod(TORUS)
    return steps


def spectral_tables(steps):
    half = steps // 2
    t = np.arange(steps)[:, None]
    even = 2 * np.arange(half + 1)[None, :]
    odd = 2 * np.arange(half)[None, :] + 1
    turn = math.pi / steps
    even_re = np.cos(turn * (t * even % (2 * steps)))
    even_im = -np.sin(turn * (t * even % (2 * steps)))
    even_im[:, 0] = np.arange(steps) == 0
    even_im[:, half] = 0.0
    odd_re = np.cos(turn * (t * odd % (2 * steps)))
    odd_im = -np.sin(turn * (t * odd % (2 * steps)))
    forward = np.zeros((512, 512))
    forward[:steps, : half + 1] = even_re
    forward[:steps, 256 : 256 + half + 1] = even_im
    weight = np.full((half + 1,), 2.0 / steps)
    weight[0] = weight[half] = 1.0 / steps
    across = np.zeros((2, 256, 256))
    across[0, : half + 1, :half] = weight[:, None] * (even_re.T @ odd_im)
    across[1, : half + 1, :half] = weight[:, None] * (even_im.T @ odd_re)
    across[1, 0, :half] = 1.0
    gains = np.zeros((8, 512))
    gains[0, : half + 1] = weight / 2
    gains[0, 256 : 256 + half] = 1.0 / steps
    gains[1] = gains[0]
    gains[1, 0] = 0.0
    return (forward, across, gains)


def high_low(array):
    array = array.astype(np.float32)
    high = array.astype(jnp.bfloat16)
    low = (array - high.astype(np.float32)).astype(jnp.bfloat16)
    return (high, low)


def split(value):
    high = value.astype(BF16)
    return (high, (value - high.astype(F32)).astype(BF16))


def times(value, high, low, transposed=False):
    dims = (((1,), (1 if transposed else 0,)), ((), ()))
    dot = functools.partial(lax.dot_general, dimension_numbers=dims, preferred_element_type=F32)
    upper, lower = split(value)
    return dot(upper, high) + dot(lower, high) + dot(upper, low)


def kernel(
    steps,
    data_ref,
    k_ref,
    fh_ref,
    fl_ref,
    ah_ref,
    al_ref,
    gain_ref,
    field_ref,
    rms_ref,
    gat,
    xv,
    xs,
    kraw,
    kt,
    fh,
    fl,
    ah,
    al,
    gain,
    eb,
    do,
    acc,
    part,
    other,
    red1,
    red2,
    srow,
    send_sem,
    recv_sem,
    load_sem,
    pair_sem,
    red_sem,
):
    vectors, own, length = data_ref.shape
    me = tuple(lax.axis_index(name) for name in PARAM)
    core = lax.axis_index("sensor")

    def device(offset):
        return {
            name: lax.rem(pos + (o % n), n) for name, pos, o, n in zip(PARAM, me, offset, TORUS)
        }

    beside = [device(offset) for offset in DIRS]
    partner = {"sensor": 1 - core}
    barrier = pltpu.get_barrier_semaphore()
    for offset in DIRS + (tuple(-o for o in EXTRA),):
        pl.semaphore_signal(barrier, inc=1, device_id=device(offset), device_id_type=MESH)
    pl.semaphore_signal(barrier, inc=1, device_id=partner, device_id_type=MESH)

    rows_k = k_ref.shape[1]
    loads = [
        pltpu.make_async_copy(data_ref, xv, load_sem.at[0]),
        pltpu.make_async_copy(fh_ref, fh, load_sem.at[1]),
        pltpu.make_async_copy(fl_ref, fl, load_sem.at[2]),
        pltpu.make_async_copy(k_ref, kraw.at[:, pl.ds(0, rows_k), :], load_sem.at[3]),
        pltpu.make_async_copy(ah_ref, ah, load_sem.at[4]),
        pltpu.make_async_copy(al_ref, al, load_sem.at[5]),
        pltpu.make_async_copy(gain_ref, gain, load_sem.at[6]),
    ]
    for load in loads:
        load.start()

    slot_of = {(0, 0, 0): 0, EXTRA: 1}
    for k, step in enumerate(steps):
        for i, (d, p, c) in enumerate(step):
            slot_of[c] = 2 + 6 * k + i
    step_of = {c: k for k, step in enumerate(steps, 1) for d, p, c in step}
    step_of[(0, 0, 0)] = 0
    step_of[EXTRA] = 2
    pending = {}
    for k, step in enumerate(steps):
        for d, p, c in step:
            pending.setdefault(step_of[p], []).append((d, p, c))

    def copy(source, target, count, step, where):
        return pltpu.make_async_remote_copy(
            src_ref=gat.at[pl.ds(source, count), pl.ds(0, SENT)],
            dst_ref=gat.at[pl.ds(target, count), pl.ds(0, SENT)],
            send_sem=send_sem,
            recv_sem=recv_sem.at[step],
            device_id=where,
            device_id_type=MESH,
        )

    def forward_after(k):
        for d, p, c in pending.get(k, ()):
            target = slot_of[c]
            copy(slot_of[p], target, 1, (target + 4) // 6, beside[d]).start()

    def forward_between(k, low, high):
        if high - low == 1:
            forward_after(low)
        else:
            middle = (low + high) // 2
            lax.cond(
                k < middle,
                lambda: forward_between(k, low, middle),
                lambda: forward_between(k, middle, high),
            )

    xs[:, pl.ds(384, LANES)] = jnp.zeros((2 * vectors, LANES), F32)
    loads[0].wait()
    for r in range(vectors):
        for s in range(own):
            xs[pl.ds(s * vectors + r, 1), pl.ds(0, length)] = xv[r, pl.ds(s, 1), :]
    loads[1].wait()
    loads[2].wait()
    spec = times(xs[...], fh[...], fl[...])
    lane = lax.broadcasted_iota(jnp.int32, (32, LANES), 1)
    lane8 = lax.broadcasted_iota(jnp.int32, (8, LANES), 1)
    re_b = spec[:, 128:256]
    im_b = spec[:, 384:512]
    gat[0, pl.ds(0, 32), :] = spec[:, 0:128]
    gat[0, pl.ds(32, 32), :] = spec[:, 256:384]
    gat[0, pl.ds(64, 32), :] = re_b + pltpu.roll(
        jnp.where(lane < PIECE, im_b, 0.0), LANES - PIECE, 1
    )
    rest = jnp.where((lane >= PIECE) & (lane < PIECE + REST), im_b, 0.0)
    groups = [
        pltpu.roll(rest[8 * g : 8 * g + 8], (REST * (g % 3) - PIECE) % LANES, 1) for g in range(4)
    ]
    gat[0, pl.ds(96, 8), :] = groups[0] + groups[1] + groups[2]
    row8 = lax.broadcasted_iota(jnp.int32, (8, LANES), 0)
    folded = jnp.where(row8 < 3, groups[3], 0.0)
    for i in (1, 2):
        third = jnp.where((row8 >= 3 * i) & (row8 < 3 * i + 3), groups[3], 0.0)
        folded = folded + pltpu.roll(pltpu.roll(third, 8 - 3 * i, 0), REST * i, 1)
    gat[0, pl.ds(104, 8), :] = folded

    pl.semaphore_wait(barrier, 8)
    forward_after(0)
    copy(0, 1, 1, 0, device(EXTRA)).start()

    for offset, slot in slot_of.items():
        z, x, y = (
            lax.rem(pos + n - o, n) for pos, o, n in zip(me, offset, TORUS)
        )
        srow[slot] = ((z * TORUS[1] + x) * TORUS[2] + y) * own * 8

    acc[...] = jnp.zeros(acc.shape, F32)
    for c in range(2):
        tail_rows = kraw.shape[1] - rows_k
        kraw[c, pl.ds(rows_k, tail_rows), :] = jnp.zeros((tail_rows, LANES), F32)
    loads[3].wait()
    loads[4].wait()
    loads[5].wait()
    loads[6].wait()

    def transpose_tile(ft):
        parity, half = divmod(ft, 2)
        base = (2 * half * LANES + parity) * 8

        @pl.loop(0, 8)
        def _(i):
            st = i // 4
            p = lax.rem(i, 4)
            for c in range(2):
                block = kraw[c, pl.ds(base + st * 4 + p, LANES, stride=16), :]
                turned = block.T
                if c == 1 and ft == 0:
                    first = lax.broadcasted_iota(jnp.int32, (LANES, LANES), 1) == 0
                    turned = jnp.where(first, 0.0, turned)
                kt[ft, pl.ds(st * LANES * 8 + c * 4 + p, LANES, stride=8), :] = turned


    def consume(first, count):
        number = 32 * count
        for j in range(count):
            tile2 = gat[first + j, pl.ds(64, 32), :]
            left = gat[first + j, pl.ds(96, 16), :]
            moved2 = pltpu.roll(tile2, PIECE, 1)
            for g in range(4):
                if g < 3:
                    back = pltpu.roll(left[0:8], (PIECE - REST * g) % LANES, 1)
                else:
                    thirds = [
                        pltpu.roll(left[8:16], (PIECE - REST * i) % LANES, 1) for i in range(3)
                    ]
                    back = jnp.where(
                        row8 < 3,
                        thirds[0],
                        jnp.where(row8 < 6, pltpu.roll(thirds[1], 3, 0), pltpu.roll(thirds[2], 6, 0)),
                    )
                value = jnp.where(
                    lane8 < PIECE,
                    moved2[8 * g : 8 * g + 8],
                    jnp.where(lane8 < PIECE + REST, back, 0.0),
                )
                eb[pl.ds(32 * j + 8 * g, 8), :] = value

        def tiles(row):
            return gat[pl.ds(first, count), pl.ds(row, 32), :].reshape(number, LANES)

        even_re = jnp.concatenate([tiles(0), tiles(64)], axis=1)
        do[pl.ds(0, number), pl.ds(256, 256)] = times(even_re, ah[0], al[0])
        even_im = jnp.concatenate([tiles(32), eb[pl.ds(0, number), :]], axis=1)
        do[pl.ds(0, number), pl.ds(0, 256)] = times(even_im, ah[1], al[1])

        def d_value(ft, j, s, h, imag):
            inner = s * 16 + h * 8
            if ft == 0:
                return gat[first + j, pl.ds((32 if imag else 0) + inner, 8), :]
            if ft == 1:
                if imag:
                    return eb[pl.ds(pl.multiple_of(j * 32 + inner, 8), 8), :]
                return gat[first + j, pl.ds(64 + inner, 8), :]
            return do[
                pl.ds(pl.multiple_of(j * 32 + inner, 8), 8),
                pl.ds((256 if imag else 0) + (ft - 2) * LANES, LANES),
            ]

        for ft in range(4):
            start = tuple(
                acc[c, pl.ds(p * 16 + h * 8, 8), pl.ds(ft * LANES, LANES)]
                for c in range(2)
                for p in range(4)
                for h in range(2)
            )

            def sensors(j, sums):
                sums = list(sums)
                row = srow[first + j]
                for s in range(own):
                    d_re = [d_value(ft, j, s, h, False) for h in range(2)]
                    d_im = [d_value(ft, j, s, h, True) for h in range(2)]
                    for p in range(4):
                        at = pl.multiple_of(row + s * 8, 8)
                        k_re = jnp.broadcast_to(kt[ft, pl.ds(at + p, 1), :], (8, LANES))
                        k_im = jnp.broadcast_to(kt[ft, pl.ds(at + 4 + p, 1), :], (8, LANES))
                        for h in range(2):
                            i = p * 2 + h
                            sums[i] = sums[i] + k_re * d_re[h] + k_im * d_im[h]
                            sums[8 + i] = sums[8 + i] + k_re * d_im[h] - k_im * d_re[h]
                return tuple(sums)

            final = lax.fori_loop(0, count, sensors, start, unroll=UNROLL if count % UNROLL == 0 else 1)
            for i, value in enumerate(final):
                c, p, h = i // 8, i // 2 % 4, i % 2
                acc[c, pl.ds(p * 16 + h * 8, 8), pl.ds(ft * LANES, LANES)] = value

    for ft in range(3):
        transpose_tile(ft)
    last = len(steps)

    @pl.loop(1, last + 1)
    def _(k):
        copy(0, 6 * k - 4, 6, k, beside[0]).wait_recv()

        @pl.when(k == 2)
        def _():
            copy(0, 1, 1, 0, beside[0]).wait_recv()

        @pl.when(k < last)
        def _():
            forward_between(k, 1, last)

        @pl.when(k == 1)
        def _():
            transpose_tile(3)

        @pl.when(k == 2)
        def _():
            consume(0, 2)

        low = jnp.where(k == 2, 0, k - 1)
        high = jnp.where(k == 1, 0, k)

        @pl.loop(low, high)
        def _(b):
            consume(2 + 6 * b, 6)

    out_re = acc[0] * gain[0:1, :]
    out_im = acc[1] * gain[1:2, :]
    s_re = out_re[:, 0:256] + times(out_im[:, 256:512], ah[0], al[0], True)
    s_im = out_im[:, 0:256] + times(out_re[:, 256:512], ah[1], al[1], True)
    total = times(s_re, fh[:, 0:256], fl[:, 0:256], True) + times(
        s_im, fh[:, 256:512], fl[:, 256:512], True
    )
    part[...] = total
    swap = pltpu.make_async_remote_copy(
        src_ref=part,
        dst_ref=other,
        send_sem=pair_sem.at[0],
        recv_sem=pair_sem.at[1],
        device_id=partner,
        device_id_type=MESH,
    )
    swap.start()
    copy(1, 1, gat.shape[0] - 1, 0, beside[0]).wait_send()
    swap.wait()
    field = part[...] + other[...]
    square = field * field
    square = square[:, 0:128] + square[:, 128:256] + square[:, 256:384] + square[:, 384:512]
    square = square[0:16] + square[16:32] + square[32:48] + square[48:64]
    diagonal = lax.broadcasted_iota(jnp.int32, (16, LANES), 0) == lax.broadcasted_iota(
        jnp.int32, (16, LANES), 1
    )
    column = jnp.sum(square, axis=1, keepdims=True)
    z, x, y = me
    spot = x * TORUS[2] + y
    red1[spot] = jnp.sum(jnp.where(diagonal, column, 0.0), axis=0, keepdims=True)

    def spread(ref, mine, first, offsets):
        sends = [
            pltpu.make_async_remote_copy(
                src_ref=ref.at[pl.ds(mine, 1)],
                dst_ref=ref.at[pl.ds(mine, 1)],
                send_sem=red_sem.at[first],
                recv_sem=red_sem.at[first + 1],
                device_id=device(offset),
                device_id_type=MESH,
            )
            for offset in offsets
        ]
        for send in sends:
            send.start()
        every = ref.at[pl.ds(0, len(offsets))]
        whole = pltpu.make_async_remote_copy(
            src_ref=every,
            dst_ref=every,
            send_sem=red_sem.at[first],
            recv_sem=red_sem.at[first + 1],
            device_id=beside[0],
            device_id_type=MESH,
        )
        whole.wait()
        total = ref[0]
        for i in range(1, len(offsets) + 1):
            total = total + ref[i]
        return total

    plane = [(0, dx, dy) for dx in range(TORUS[1]) for dy in range(TORUS[2]) if dx + dy > 0]
    red2[z] = spread(red1, spot, 0, plane)
    whole = spread(red2, z, 2, [(dz, 0, 0) for dz in range(1, TORUS[0])])
    count = 4 * math.prod(TORUS) * length
    rms = jnp.sqrt(whole / count + 1e-6)
    rms_ref[...] = rms
    column = jnp.sum(jnp.where(diagonal, 1.0 / rms, 0.0), axis=1, keepdims=True)
    for p in range(4):
        field_ref[:, p, :] = field[16 * p : 16 * p + 16, 0:length] * column


def body(data, spectra):
    vectors, own, length = data.shape
    freqs = length + 1
    sensors = spectra.shape[1]
    points = spectra.shape[2]
    forward, across, gains = spectral_tables(length)
    fh, fl = high_low(forward)
    ah, al = high_low(across)
    k_rows = jnp.transpose(
        spectra.reshape(2, sensors // LANES, LANES, points, freqs), (0, 4, 1, 3, 2)
    ).reshape(2, freqs * 8, LANES)
    steps = make_schedule()
    devices = math.prod(TORUS)
    vmem = pltpu.VMEM
    field, rms = pl.pallas_call(
        functools.partial(kernel, steps),
        out_shape=(
            pltpu.VMEM((vectors, points, length), F32),
            pltpu.VMEM((1, LANES), F32),
        ),
        in_specs=[pl.BlockSpec(memory_space=pltpu.HBM)] * 7,
        out_specs=[pl.BlockSpec(memory_space=pltpu.VMEM)] * 2,
        scratch_shapes=[
            vmem((devices, ROWS, LANES), F32),
            vmem((vectors, own, length), F32),
            vmem((vectors * own, 512), F32),
            vmem((2, 4096, LANES), F32),
            vmem((4, sensors * 8, LANES), F32),
            vmem((512, 512), BF16),
            vmem((512, 512), BF16),
            vmem((2, 256, 256), BF16),
            vmem((2, 256, 256), BF16),
            vmem((8, 512), F32),
            vmem((192, LANES), F32),
            vmem((192, 512), F32),
            vmem((2, points * vectors, 512), F32),
            vmem((points * vectors, 512), F32),
            vmem((points * vectors, 512), F32),
            vmem((16, 1, LANES), F32),
            vmem((8, 1, LANES), F32),
            pltpu.SMEM((devices,), jnp.int32),
            pltpu.SemaphoreType.DMA,
            pltpu.SemaphoreType.DMA((len(steps) + 1,)),
            pltpu.SemaphoreType.DMA((7,)),
            pltpu.SemaphoreType.DMA((2,)),
            pltpu.SemaphoreType.DMA((4,)),
        ],
        compiler_params=pltpu.CompilerParams(
            collective_id=0, has_side_effects=True, vmem_limit_bytes=VMEM_LIMIT
        ),
        name="adjoint",
    )(data, k_rows, jnp.asarray(fh), jnp.asarray(fl), jnp.asarray(ah), jnp.asarray(al), jnp.asarray(gains, F32))
    return (field, rms[0, :vectors])


def solution(mesh):
    split_mesh = Mesh(
        mesh.devices.reshape(*TORUS, mesh.shape["sensor"]), (*PARAM, "sensor")
    )
    placed = (P(None, SENSOR_PARAM, None), P(None, "sensor", PARAM, None))
    return jax.shard_map(
        body, mesh=split_mesh, in_specs=placed, out_specs=(P(None, PARAM, None), P()), check_vma=False
    )
```

```python
import functools
import math

import jax
import jax.numpy as jnp
import numpy as np
from jax import lax
from jax.experimental import pallas as pl
from jax.experimental.pallas import tpu as pltpu
from jax.sharding import Mesh
from jax.sharding import PartitionSpec as P

PARAM = ("param_0", "param_1", "param_2")
SENSOR_PARAM = ("sensor", "param_0", "param_1", "param_2")
MESH = pl.DeviceIdType.MESH
F32 = jnp.float32
BF16 = jnp.bfloat16
TORUS = (8, 4, 4)
VECTORS = (
    (0, 1, 0),
    (0, -1, 0),
    (0, 0, 1),
    (0, 0, -1),
    (1, 0, 0),
    (-1, 0, 0),
    (-1, 0, 1),
    (0, -1, -1),
    (1, 1, 0),
)
COPIES = (
    (0, 0, 0, 3), (0, 0, 1, 4), (0, 0, 2, 1), (0, 0, 3, 2), (0, 0, 4, 5),
    (0, 0, 5, 6), (1, 2, 0, 8), (1, 6, 1, 12), (1, 5, 2, 9), (1, 2, 3, 7),
    (1, 6, 5, 11), (1, 5, 4, 10), (1, 6, 3, 17), (1, 3, 5, 18), (1, 4, 4, 16),
    (1, 3, 2, 13), (1, 4, 1, 14), (1, 5, 0, 15), (1, 2, 1, 20), (1, 5, 3, 21),
    (1, 4, 2, 19), (1, 1, 5, 22), (2, 8, 8, 23), (2, 11, 6, 24), (2, 12, 7, 25),
    (2, 10, 4, 28), (2, 11, 3, 30), (2, 11, 5, 29), (2, 11, 0, 31), (2, 10, 1, 27),
    (2, 10, 2, 26), (2, 12, 5, 37), (2, 10, 0, 35), (2, 11, 2, 36), (2, 7, 1, 32),
    (2, 10, 3, 34), (2, 7, 4, 33), (3, 8, 3, 38), (3, 18, 2, 43), (3, 9, 0, 39),
    (3, 7, 5, 42), (3, 9, 1, 41), (3, 8, 4, 40), (4, 24, 2, 47), (4, 24, 0, 48),
    (4, 24, 5, 46), (4, 23, 4, 45), (4, 24, 1, 49), (4, 23, 3, 44), (4, 13, 0, 50),
    (4, 22, 1, 54), (4, 8, 5, 53), (4, 12, 3, 55), (4, 14, 4, 51), (4, 23, 0, 57),
    (4, 14, 3, 56), (4, 14, 5, 61), (5, 27, 2, 52), (5, 27, 4, 59), (5, 26, 2, 58),
    (5, 30, 1, 60), (6, 25, 3, 67), (6, 28, 2, 63), (6, 29, 1, 65), (6, 35, 4, 64),
    (6, 26, 0, 62), (6, 25, 5, 66), (7, 29, 0, 72), (7, 28, 3, 69), (7, 31, 2, 73),
    (7, 28, 4, 70), (7, 34, 1, 68), (7, 30, 5, 71), (8, 45, 4, 75), (8, 48, 0, 79),
    (8, 46, 2, 76), (8, 46, 1, 78), (8, 48, 5, 77), (8, 45, 3, 74), (9, 47, 0, 83),
    (9, 52, 4, 82), (9, 49, 2, 84), (9, 54, 5, 85), (9, 35, 3, 80), (9, 52, 1, 81),
    (10, 42, 5, 90), (10, 59, 1, 88), (10, 31, 3, 91), (10, 58, 0, 86), (10, 59, 4, 89),
    (10, 52, 2, 87), (11, 63, 0, 92), (11, 66, 2, 96), (11, 66, 3, 97), (11, 65, 1, 94),
    (11, 64, 4, 93), (11, 66, 5, 95), (12, 68, 4, 100), (12, 54, 1, 103), (12, 63, 2, 98),
    (12, 71, 5, 101), (12, 64, 3, 99), (12, 42, 0, 102), (13, 75, 3, 104), (13, 77, 0, 106),
    (13, 77, 2, 105), (13, 75, 4, 107), (13, 76, 1, 108), (13, 60, 5, 109), (14, 84, 4, 114),
    (14, 72, 3, 111), (14, 79, 2, 112), (14, 32, 5, 115), (14, 73, 0, 113), (14, 32, 1, 110),
    (15, 89, 3, 121), (15, 88, 2, 118), (15, 33, 0, 116), (15, 87, 4, 119), (15, 87, 5, 117),
    (15, 89, 1, 120), (16, 83, 4, 126), (16, 81, 5, 122), (16, 92, 2, 124), (16, 35, 0, 123),
    (16, 93, 3, 125), (18, 108, 1, 127),
)
ROWS = 112
SENT = 107
GROUP = 6
LANES = 128
PIECE = 45
REST = 37
VMEM_LIMIT = 66_000_000


def moved(offset, step):
    return tuple((a + b) % n for a, b, n in zip(offset, step, TORUS))


def spectral_tables(steps):
    half = steps // 2
    t = np.arange(steps)[:, None]
    even = 2 * np.arange(half + 1)[None, :]
    odd = 2 * np.arange(half)[None, :] + 1
    turn = math.pi / steps
    even_re = np.cos(turn * (t * even % (2 * steps)))
    even_im = -np.sin(turn * (t * even % (2 * steps)))
    even_im[:, 0] = np.arange(steps) == 0
    even_im[:, half] = 0.0
    odd_re = np.cos(turn * (t * odd % (2 * steps)))
    odd_im = -np.sin(turn * (t * odd % (2 * steps)))
    forward = np.zeros((512, 512))
    forward[:steps, : half + 1] = even_re
    forward[:steps, 256 : 256 + half + 1] = even_im
    weight = np.full((half + 1,), 2.0 / steps)
    weight[0] = weight[half] = 1.0 / steps
    across = np.zeros((2, 256, 256))
    across[0, : half + 1, :half] = weight[:, None] * (even_re.T @ odd_im)
    across[1, : half + 1, :half] = weight[:, None] * (even_im.T @ odd_re)
    across[1, 0, :half] = 1.0
    gains = np.zeros((8, 512))
    gains[0, : half + 1] = weight / 2
    gains[0, 256 : 256 + half] = 1.0 / steps
    gains[1] = gains[0]
    gains[1, 0] = 0.0
    return (forward, across, gains)


def high_low(array):
    array = array.astype(np.float32)
    high = array.astype(jnp.bfloat16)
    low = (array - high.astype(np.float32)).astype(jnp.bfloat16)
    return (high, low)


def split(value):
    high = value.astype(BF16)
    return (high, (value - high.astype(F32)).astype(BF16))


def times(value, high, low, transposed=False):
    dims = (((1,), (1 if transposed else 0,)), ((), ()))
    dot = functools.partial(lax.dot_general, dimension_numbers=dims, preferred_element_type=F32)
    upper, lower = split(value)
    return dot(upper, high) + dot(lower, high) + dot(upper, low)


def kernel(
    data_ref,
    k_ref,
    fh_ref,
    fl_ref,
    ah_ref,
    al_ref,
    gain_ref,
    field_ref,
    rms_ref,
    gat,
    xv,
    xs,
    kraw,
    kt,
    fh,
    fl,
    ah,
    al,
    gain,
    eb,
    do,
    acc,
    part,
    other,
    red1,
    red2,
    srow,
    send_sem,
    recv_sem,
    load_sem,
    pair_sem,
    red_sem,
):
    vectors, own, length = data_ref.shape
    me = tuple(lax.axis_index(name) for name in PARAM)
    core = lax.axis_index("sensor")

    def device(offset):
        return {
            name: lax.rem(pos + (o % n), n) for name, pos, o, n in zip(PARAM, me, offset, TORUS)
        }

    beside = [device(offset) for offset in VECTORS]
    partner = {"sensor": 1 - core}
    barrier = pltpu.get_barrier_semaphore()
    for where in beside[:6]:
        pl.semaphore_signal(barrier, inc=1, device_id=where, device_id_type=MESH)
    pl.semaphore_signal(barrier, inc=1, device_id=partner, device_id_type=MESH)

    rows_k = k_ref.shape[1]
    loads = [
        pltpu.make_async_copy(data_ref, xv, load_sem.at[0]),
        pltpu.make_async_copy(fh_ref, fh, load_sem.at[1]),
        pltpu.make_async_copy(fl_ref, fl, load_sem.at[2]),
        pltpu.make_async_copy(k_ref, kraw.at[:, pl.ds(0, rows_k), :], load_sem.at[3]),
        pltpu.make_async_copy(ah_ref, ah, load_sem.at[4]),
        pltpu.make_async_copy(al_ref, al, load_sem.at[5]),
        pltpu.make_async_copy(gain_ref, gain, load_sem.at[6]),
    ]
    for load in loads:
        load.start()

    offsets = {0: (0, 0, 0)}
    for _, source, vector, target in COPIES:
        offsets[target] = moved(offsets[source], VECTORS[vector])
    last = (len(COPIES) - 1) // GROUP + 1
    rest_of = len(COPIES) - GROUP * (last - 1)

    def copy(source, target, count, step, where):
        return pltpu.make_async_remote_copy(
            src_ref=gat.at[pl.ds(source, count), pl.ds(0, SENT)],
            dst_ref=gat.at[pl.ds(target, count), pl.ds(0, SENT)],
            send_sem=send_sem,
            recv_sem=recv_sem.at[step],
            device_id=where,
            device_id_type=MESH,
        )

    def forward_after(k):
        for when, source, vector, target in COPIES:
            if when == k:
                copy(source, target, 1, (target - 1) // GROUP, beside[vector]).start()

    def forward_between(k, low, high):
        if high - low == 1:
            forward_after(low)
        else:
            middle = (low + high) // 2
            lax.cond(
                k < middle,
                lambda: forward_between(k, low, middle),
                lambda: forward_between(k, middle, high),
            )

    xs[:, pl.ds(384, LANES)] = jnp.zeros((2 * vectors, LANES), F32)
    loads[0].wait()
    for r in range(vectors):
        for s in range(own):
            xs[pl.ds(s * vectors + r, 1), pl.ds(0, length)] = xv[r, pl.ds(s, 1), :]
    loads[1].wait()
    loads[2].wait()
    spec = times(xs[...], fh[...], fl[...])
    lane = lax.broadcasted_iota(jnp.int32, (32, LANES), 1)
    lane8 = lax.broadcasted_iota(jnp.int32, (8, LANES), 1)
    re_b = spec[:, 128:256]
    im_b = spec[:, 384:512]
    gat[0, pl.ds(0, 32), :] = spec[:, 0:128]
    gat[0, pl.ds(32, 32), :] = spec[:, 256:384]
    gat[0, pl.ds(64, 32), :] = re_b + pltpu.roll(
        jnp.where(lane < PIECE, im_b, 0.0), LANES - PIECE, 1
    )
    rest = jnp.where((lane >= PIECE) & (lane < PIECE + REST), im_b, 0.0)
    groups = [
        pltpu.roll(rest[8 * g : 8 * g + 8], (REST * (g % 3) - PIECE) % LANES, 1) for g in range(4)
    ]
    gat[0, pl.ds(96, 8), :] = groups[0] + groups[1] + groups[2]
    row8 = lax.broadcasted_iota(jnp.int32, (8, LANES), 0)
    folded = jnp.where(row8 < 3, groups[3], 0.0)
    for i in (1, 2):
        third = jnp.where((row8 >= 3 * i) & (row8 < 3 * i + 3), groups[3], 0.0)
        folded = folded + pltpu.roll(pltpu.roll(third, 8 - 3 * i, 0), REST * i, 1)
    gat[0, pl.ds(104, 8), :] = folded

    pl.semaphore_wait(barrier, 7)
    forward_after(0)
    for slot, offset in offsets.items():
        z, x, y = (
            lax.rem(pos + n - o, n) for pos, o, n in zip(me, offset, TORUS)
        )
        srow[slot] = ((z * TORUS[1] + x) * TORUS[2] + y) * own * 8

    acc[...] = jnp.zeros(acc.shape, F32)
    for c in range(2):
        tail_rows = kraw.shape[1] - rows_k
        kraw[c, pl.ds(rows_k, tail_rows), :] = jnp.zeros((tail_rows, LANES), F32)
    loads[3].wait()
    loads[4].wait()
    loads[5].wait()
    loads[6].wait()

    def transpose_tile(ft):
        parity, half = divmod(ft, 2)
        base = (2 * half * LANES + parity) * 8

        @pl.loop(0, 8)
        def _(i):
            st = i // 4
            p = lax.rem(i, 4)
            for c in range(2):
                block = kraw[c, pl.ds(base + st * 4 + p, LANES, stride=16), :]
                turned = block.T
                if c == 1 and ft == 0:
                    first = lax.broadcasted_iota(jnp.int32, (LANES, LANES), 1) == 0
                    turned = jnp.where(first, 0.0, turned)
                kt[ft, pl.ds(st * LANES * 8 + c * 4 + p, LANES, stride=8), :] = turned


    def consume(first, count):
        number = 32 * count
        for j in range(count):
            tile2 = gat[first + j, pl.ds(64, 32), :]
            left = gat[first + j, pl.ds(96, 16), :]
            moved2 = pltpu.roll(tile2, PIECE, 1)
            for g in range(4):
                if g < 3:
                    back = pltpu.roll(left[0:8], (PIECE - REST * g) % LANES, 1)
                else:
                    thirds = [
                        pltpu.roll(left[8:16], (PIECE - REST * i) % LANES, 1) for i in range(3)
                    ]
                    back = jnp.where(
                        row8 < 3,
                        thirds[0],
                        jnp.where(row8 < 6, pltpu.roll(thirds[1], 3, 0), pltpu.roll(thirds[2], 6, 0)),
                    )
                value = jnp.where(
                    lane8 < PIECE,
                    moved2[8 * g : 8 * g + 8],
                    jnp.where(lane8 < PIECE + REST, back, 0.0),
                )
                eb[pl.ds(32 * j + 8 * g, 8), :] = value

        def tiles(row):
            return gat[pl.ds(first, count), pl.ds(row, 32), :].reshape(number, LANES)

        even_re = jnp.concatenate([tiles(0), tiles(64)], axis=1)
        do[pl.ds(0, number), pl.ds(256, 256)] = times(even_re, ah[0], al[0])
        even_im = jnp.concatenate([tiles(32), eb[pl.ds(0, number), :]], axis=1)
        do[pl.ds(0, number), pl.ds(0, 256)] = times(even_im, ah[1], al[1])

        def d_value(ft, j, s, h, imag):
            inner = s * 16 + h * 8
            if ft == 0:
                return gat[first + j, pl.ds((32 if imag else 0) + inner, 8), :]
            if ft == 1:
                if imag:
                    return eb[pl.ds(pl.multiple_of(j * 32 + inner, 8), 8), :]
                return gat[first + j, pl.ds(64 + inner, 8), :]
            return do[
                pl.ds(pl.multiple_of(j * 32 + inner, 8), 8),
                pl.ds((256 if imag else 0) + (ft - 2) * LANES, LANES),
            ]

        for ft in range(4):
            start = tuple(
                acc[c, pl.ds(p * 16 + h * 8, 8), pl.ds(ft * LANES, LANES)]
                for c in range(2)
                for p in range(4)
                for h in range(2)
            )

            def sensors(j, sums):
                sums = list(sums)
                row = srow[first + j]
                for s in range(own):
                    d_re = [d_value(ft, j, s, h, False) for h in range(2)]
                    d_im = [d_value(ft, j, s, h, True) for h in range(2)]
                    for p in range(4):
                        at = pl.multiple_of(row + s * 8, 8)
                        k_re = jnp.broadcast_to(kt[ft, pl.ds(at + p, 1), :], (8, LANES))
                        k_im = jnp.broadcast_to(kt[ft, pl.ds(at + 4 + p, 1), :], (8, LANES))
                        for h in range(2):
                            i = p * 2 + h
                            sums[i] = sums[i] + k_re * d_re[h] + k_im * d_im[h]
                            sums[8 + i] = sums[8 + i] + k_re * d_im[h] - k_im * d_re[h]
                return tuple(sums)

            final = lax.fori_loop(0, count, sensors, start, unroll=True)
            for i, value in enumerate(final):
                c, p, h = i // 8, i // 2 % 4, i % 2
                acc[c, pl.ds(p * 16 + h * 8, 8), pl.ds(ft * LANES, LANES)] = value

    for ft in range(3):
        transpose_tile(ft)

    @pl.loop(1, last)
    def _(k):
        copy(0, GROUP * k - 5, GROUP, k - 1, beside[0]).wait_recv()
        forward_between(k, 1, last)

        @pl.when(k == 1)
        def _():
            transpose_tile(3)

        @pl.when(k == 2)
        def _():
            consume(0, 1)

        low = jnp.where(k == 2, 0, k - 1)
        high = jnp.where(k == 1, 0, k)

        @pl.loop(low, high)
        def _(b):
            consume(1 + GROUP * b, GROUP)

    copy(0, GROUP * (last - 1) + 1, rest_of, last - 1, beside[0]).wait_recv()
    consume(GROUP * (last - 1) + 1, rest_of)

    out_re = acc[0] * gain[0:1, :]
    out_im = acc[1] * gain[1:2, :]
    s_re = out_re[:, 0:256] + times(out_im[:, 256:512], ah[0], al[0], True)
    s_im = out_im[:, 0:256] + times(out_re[:, 256:512], ah[1], al[1], True)
    total = times(s_re, fh[:, 0:256], fl[:, 0:256], True) + times(
        s_im, fh[:, 256:512], fl[:, 256:512], True
    )
    part[...] = total
    swap = pltpu.make_async_remote_copy(
        src_ref=part,
        dst_ref=other,
        send_sem=pair_sem.at[0],
        recv_sem=pair_sem.at[1],
        device_id=partner,
        device_id_type=MESH,
    )
    swap.start()
    copy(1, 1, gat.shape[0] - 1, 0, beside[0]).wait_send()
    swap.wait()
    field = part[...] + other[...]
    square = field * field
    square = square[:, 0:128] + square[:, 128:256] + square[:, 256:384] + square[:, 384:512]
    square = square[0:16] + square[16:32] + square[32:48] + square[48:64]
    diagonal = lax.broadcasted_iota(jnp.int32, (16, LANES), 0) == lax.broadcasted_iota(
        jnp.int32, (16, LANES), 1
    )
    z, x, y = me
    spot = x * TORUS[2] + y

    def message(ref, mine, count, first, where):
        part_of = ref.at[pl.ds(mine, count)]
        return pltpu.make_async_remote_copy(
            src_ref=part_of,
            dst_ref=part_of,
            send_sem=red_sem.at[first],
            recv_sem=red_sem.at[first + 1],
            device_id=where,
            device_id_type=MESH,
        )

    def total_of(ref):
        total = ref[0]
        for i in range(1, ref.shape[0]):
            total = total + ref[i]
        return total

    @pl.when(core == 1)
    def _():
        column = jnp.sum(square, axis=1, keepdims=True)
        red1[spot] = jnp.sum(jnp.where(diagonal, column, 0.0), axis=0, keepdims=True)
        peers = [(0, dx, dy) for dx in range(TORUS[1]) for dy in range(TORUS[2]) if dx + dy > 0]
        for offset in peers:
            message(red1, spot, 1, 0, device(offset)).start()
        message(red1, 0, len(peers), 0, beside[0]).wait()
        red2[z] = total_of(red1)
        line = [(dz, 0, 0) for dz in range(TORUS[0])]
        for offset in line[1:]:
            message(red2, z, 1, 2, device(offset)).start()
        for offset in line:
            message(red2, z, 1, 2, dict(device(offset), sensor=0)).start()
        message(red2, 0, TORUS[0] - 1, 2, beside[0]).wait_recv()
        message(red1, 0, 2 * TORUS[0] - 1, 2, beside[0]).wait_send()

    @pl.when(core == 0)
    def _():
        message(red2, 0, TORUS[0], 2, beside[0]).wait_recv()

    whole = total_of(red2)
    count = 4 * math.prod(TORUS) * length
    rms = jnp.sqrt(whole / count + 1e-6)
    rms_ref[...] = rms[0, 0:16]
    column = jnp.sum(jnp.where(diagonal, 1.0 / rms, 0.0), axis=1, keepdims=True)
    for p in range(4):
        field_ref[:, p, :] = field[16 * p : 16 * p + 16, 0:length] * column


def body(data, spectra):
    vectors, own, length = data.shape
    freqs = length + 1
    sensors = spectra.shape[1]
    points = spectra.shape[2]
    forward, across, gains = spectral_tables(length)
    fh, fl = high_low(forward)
    ah, al = high_low(across)
    k_rows = jnp.transpose(
        spectra.reshape(2, sensors // LANES, LANES, points, freqs), (0, 4, 1, 3, 2)
    ).reshape(2, freqs * 8, LANES)
    devices = math.prod(TORUS)
    vmem = pltpu.VMEM
    field, rms = pl.pallas_call(
        kernel,
        out_shape=(
            pltpu.VMEM((vectors, points, length), F32),
            pltpu.VMEM((vectors,), F32),
        ),
        in_specs=[pl.BlockSpec(memory_space=pltpu.HBM)] * 7,
        out_specs=[pl.BlockSpec(memory_space=pltpu.VMEM)] * 2,
        scratch_shapes=[
            vmem((devices, ROWS, LANES), F32),
            vmem((vectors, own, length), F32),
            vmem((vectors * own, 512), F32),
            vmem((2, 4096, LANES), F32),
            vmem((4, sensors * 8, LANES), F32),
            vmem((512, 512), BF16),
            vmem((512, 512), BF16),
            vmem((2, 256, 256), BF16),
            vmem((2, 256, 256), BF16),
            vmem((8, 512), F32),
            vmem((192, LANES), F32),
            vmem((192, 512), F32),
            vmem((2, points * vectors, 512), F32),
            vmem((points * vectors, 512), F32),
            vmem((points * vectors, 512), F32),
            vmem((16, 1, LANES), F32),
            vmem((8, 1, LANES), F32),
            pltpu.SMEM((devices,), jnp.int32),
            pltpu.SemaphoreType.DMA,
            pltpu.SemaphoreType.DMA(((len(COPIES) - 1) // GROUP + 1,)),
            pltpu.SemaphoreType.DMA((7,)),
            pltpu.SemaphoreType.DMA((2,)),
            pltpu.SemaphoreType.DMA((4,)),
        ],
        compiler_params=pltpu.CompilerParams(
            collective_id=0, has_side_effects=True, vmem_limit_bytes=VMEM_LIMIT
        ),
        name="adjoint",
    )(data, k_rows, jnp.asarray(fh), jnp.asarray(fl), jnp.asarray(ah), jnp.asarray(al), jnp.asarray(gains, F32))
    return (field, rms)


def solution(mesh):
    split_mesh = Mesh(
        mesh.devices.reshape(*TORUS, mesh.shape["sensor"]), (*PARAM, "sensor")
    )
    placed = (P(None, SENSOR_PARAM, None), P(None, "sensor", PARAM, None))
    return jax.shard_map(
        body, mesh=split_mesh, in_specs=placed, out_specs=(P(None, PARAM, None), P()), check_vma=False
    )
```

```python
import functools
import math

import jax
import jax.numpy as jnp
import numpy as np
from jax import lax
from jax.experimental import pallas as pl
from jax.experimental.pallas import tpu as pltpu
from jax.sharding import Mesh
from jax.sharding import PartitionSpec as P

PARAM = ("param_0", "param_1", "param_2")
SENSOR_PARAM = ("sensor", "param_0", "param_1", "param_2")
MESH = pl.DeviceIdType.MESH
F32 = jnp.float32
BF16 = jnp.bfloat16
TORUS = (8, 4, 4)
VECTORS = (
    (0, 1, 0),
    (0, -1, 0),
    (0, 0, 1),
    (0, 0, -1),
    (1, 0, 0),
    (-1, 0, 0),
    (-1, -1, 0),
    (-1, 0, -1),
    (0, -1, -1),
    (0, 1, -1),
    (0, 1, 1),
    (1, -1, 0),
    (1, 0, 1),
    (2, 0, 0),
)
COPIES = (
    (0, 0, 0, 3), (0, 0, 1, 4), (0, 0, 2, 1), (0, 0, 3, 2), (0, 0, 4, 5),
    (0, 0, 5, 6), (0, 0, 6, 7), (0, 0, 11, 11), (0, 0, 12, 10), (0, 0, 10, 8),
    (0, 0, 9, 9), (0, 0, 7, 12), (0, 0, 8, 17), (1, 4, 2, 13), (1, 5, 4, 15),
    (1, 5, 0, 14), (1, 6, 5, 16), (1, 5, 3, 19), (1, 4, 1, 18), (1, 6, 2, 20),
    (1, 6, 0, 21), (2, 7, 7, 25), (2, 11, 13, 31), (2, 7, 1, 24), (2, 8, 2, 22),
    (2, 10, 0, 23), (2, 12, 0, 30), (2, 11, 1, 27), (2, 12, 5, 28), (2, 12, 3, 29),
    (2, 10, 2, 26), (3, 14, 4, 35), (3, 17, 3, 33), (3, 16, 5, 36), (3, 15, 2, 34),
    (3, 17, 1, 32), (3, 16, 0, 37), (3, 15, 3, 39), (3, 15, 4, 41), (3, 16, 2, 42),
    (3, 7, 5, 43), (3, 8, 0, 38), (3, 15, 1, 40), (4, 24, 3, 49), (4, 23, 4, 46),
    (4, 24, 2, 48), (4, 22, 5, 47), (4, 19, 1, 45), (4, 23, 0, 44), (5, 27, 4, 52),
    (5, 25, 3, 55), (5, 25, 1, 54), (5, 26, 0, 50), (5, 11, 2, 51), (5, 25, 5, 53),
    (6, 31, 3, 58), (6, 36, 5, 59), (6, 31, 2, 57), (6, 31, 4, 60), (6, 36, 0, 61),
    (6, 31, 1, 56), (7, 37, 2, 66), (7, 29, 1, 67), (7, 35, 3, 63), (7, 32, 4, 62),
    (7, 41, 0, 64), (7, 42, 5, 65), (8, 47, 5, 72), (8, 46, 4, 70), (8, 42, 1, 73),
    (8, 46, 2, 68), (8, 46, 0, 69), (8, 36, 3, 71), (9, 53, 3, 78), (9, 50, 0, 74),
    (9, 48, 2, 79), (9, 53, 1, 77), (9, 39, 4, 75), (9, 53, 5, 76), (10, 59, 0, 82),
    (10, 48, 5, 85), (10, 60, 2, 84), (10, 56, 3, 81), (10, 56, 4, 83), (10, 57, 1, 80),
    (11, 58, 3, 87), (11, 66, 5, 89), (11, 55, 1, 91), (11, 61, 0, 90), (11, 62, 4, 86),
    (11, 65, 2, 88), (12, 68, 4, 93), (12, 59, 2, 94), (12, 61, 3, 96), (12, 68, 0, 92),
    (12, 65, 1, 97), (12, 72, 5, 95), (13, 34, 2, 98), (13, 76, 0, 99), (13, 70, 4, 100),
    (13, 78, 5, 102), (13, 77, 3, 103), (13, 76, 1, 101), (14, 83, 2, 109), (14, 75, 0, 107),
    (14, 57, 5, 105), (14, 26, 1, 104), (14, 34, 4, 106), (14, 81, 3, 108), (15, 82, 3, 113),
    (15, 45, 4, 110), (15, 88, 5, 112), (15, 90, 2, 114), (15, 36, 1, 115), (15, 87, 0, 111),
    (16, 42, 2, 119), (16, 85, 3, 121), (16, 92, 0, 117), (16, 95, 5, 118), (16, 96, 4, 120),
    (16, 33, 1, 116), (17, 9, 4, 123), (17, 102, 1, 124), (17, 7, 3, 127), (17, 20, 0, 125),
    (17, 13, 5, 126), (17, 1, 2, 122),
)
ROWS = 112
SENT = 107
GROUP = 6
LANES = 128
PIECE = 45
REST = 37
VMEM_LIMIT = 66_000_000


def moved(offset, step):
    return tuple((a + b) % n for a, b, n in zip(offset, step, TORUS))


def spectral_tables(steps):
    half = steps // 2
    t = np.arange(steps)[:, None]
    even = 2 * np.arange(half + 1)[None, :]
    odd = 2 * np.arange(half)[None, :] + 1
    turn = math.pi / steps
    even_re = np.cos(turn * (t * even % (2 * steps)))
    even_im = -np.sin(turn * (t * even % (2 * steps)))
    even_im[:, 0] = np.arange(steps) == 0
    even_im[:, half] = 0.0
    odd_re = np.cos(turn * (t * odd % (2 * steps)))
    odd_im = -np.sin(turn * (t * odd % (2 * steps)))
    forward = np.zeros((512, 512))
    forward[:steps, : half + 1] = even_re
    forward[:steps, 256 : 256 + half + 1] = even_im
    weight = np.full((half + 1,), 2.0 / steps)
    weight[0] = weight[half] = 1.0 / steps
    across = np.zeros((2, 256, 256))
    across[0, : half + 1, :half] = weight[:, None] * (even_re.T @ odd_im)
    across[1, : half + 1, :half] = weight[:, None] * (even_im.T @ odd_re)
    across[1, 0, :half] = 1.0
    gains = np.zeros((8, 512))
    gains[0, : half + 1] = weight / 2
    gains[0, 256 : 256 + half] = 1.0 / steps
    gains[1] = gains[0]
    gains[1, 0] = 0.0
    return (forward, across, gains)


def high_low(array):
    array = array.astype(np.float32)
    high = array.astype(jnp.bfloat16)
    low = (array - high.astype(np.float32)).astype(jnp.bfloat16)
    return (high, low)


def split(value):
    high = value.astype(BF16)
    return (high, (value - high.astype(F32)).astype(BF16))


def times(value, high, low, transposed=False):
    dims = (((1,), (1 if transposed else 0,)), ((), ()))
    dot = functools.partial(lax.dot_general, dimension_numbers=dims, preferred_element_type=F32)
    upper, lower = split(value)
    return dot(upper, high) + dot(lower, high) + dot(upper, low)


def kernel(
    data_ref,
    k_ref,
    fh_ref,
    fl_ref,
    ah_ref,
    al_ref,
    gain_ref,
    field_ref,
    rms_ref,
    gat,
    xv,
    xs,
    kraw,
    kt,
    fh,
    fl,
    ah,
    al,
    gain,
    eb,
    do,
    acc,
    part,
    other,
    red1,
    red2,
    srow,
    send_sem,
    recv_sem,
    load_sem,
    pair_sem,
    red_sem,
    ready_sem,
):
    vectors, own, length = data_ref.shape
    me = tuple(lax.axis_index(name) for name in PARAM)
    core = lax.axis_index("sensor")

    def device(offset):
        return {
            name: lax.rem(pos + (o % n), n) for name, pos, o, n in zip(PARAM, me, offset, TORUS)
        }

    beside = [device(offset) for offset in VECTORS]
    partner = {"sensor": 1 - core}
    barrier = pltpu.get_barrier_semaphore()
    for where in beside[:6]:
        pl.semaphore_signal(barrier, inc=1, device_id=where, device_id_type=MESH)
    pl.semaphore_signal(barrier, inc=1, device_id=partner, device_id_type=MESH)

    rows_k = k_ref.shape[1]
    loads = [
        pltpu.make_async_copy(data_ref, xv, load_sem.at[0]),
        pltpu.make_async_copy(fh_ref, fh, load_sem.at[1]),
        pltpu.make_async_copy(fl_ref, fl, load_sem.at[2]),
        pltpu.make_async_copy(k_ref, kraw.at[:, pl.ds(0, rows_k), :], load_sem.at[3]),
        pltpu.make_async_copy(ah_ref, ah, load_sem.at[4]),
        pltpu.make_async_copy(al_ref, al, load_sem.at[5]),
        pltpu.make_async_copy(gain_ref, gain, load_sem.at[6]),
    ]
    for load in loads:
        load.start()

    offsets = {0: (0, 0, 0)}
    for _, source, vector, target in COPIES:
        offsets[target] = moved(offsets[source], VECTORS[vector])
    last = (len(COPIES) - 1) // GROUP + 1
    rest_of = len(COPIES) - GROUP * (last - 1)

    def copy(source, target, count, step, where):
        return pltpu.make_async_remote_copy(
            src_ref=gat.at[pl.ds(source, count), pl.ds(0, SENT)],
            dst_ref=gat.at[pl.ds(target, count), pl.ds(0, SENT)],
            send_sem=send_sem,
            recv_sem=recv_sem.at[step],
            device_id=where,
            device_id_type=MESH,
        )

    def forward_after(k, near=True, far=True):
        for when, source, vector, target in COPIES:
            if when == k and (near if vector < 6 else far):
                copy(source, target, 1, (target - 1) // GROUP, beside[vector]).start()

    def forward_between(k, low, high):
        if high - low == 1:
            forward_after(low)
        else:
            middle = (low + high) // 2
            lax.cond(
                k < middle,
                lambda: forward_between(k, low, middle),
                lambda: forward_between(k, middle, high),
            )

    xs[:, pl.ds(384, LANES)] = jnp.zeros((2 * vectors, LANES), F32)
    loads[0].wait()
    for r in range(vectors):
        for s in range(own):
            xs[pl.ds(s * vectors + r, 1), pl.ds(0, length)] = xv[r, pl.ds(s, 1), :]
    loads[1].wait()
    loads[2].wait()
    spec = times(xs[...], fh[...], fl[...])
    lane = lax.broadcasted_iota(jnp.int32, (32, LANES), 1)
    lane8 = lax.broadcasted_iota(jnp.int32, (8, LANES), 1)
    re_b = spec[:, 128:256]
    im_b = spec[:, 384:512]
    gat[0, pl.ds(0, 32), :] = spec[:, 0:128]
    gat[0, pl.ds(32, 32), :] = spec[:, 256:384]
    gat[0, pl.ds(64, 32), :] = re_b + pltpu.roll(
        jnp.where(lane < PIECE, im_b, 0.0), LANES - PIECE, 1
    )
    rest = jnp.where((lane >= PIECE) & (lane < PIECE + REST), im_b, 0.0)
    groups = [
        pltpu.roll(rest[8 * g : 8 * g + 8], (REST * (g % 3) - PIECE) % LANES, 1) for g in range(4)
    ]
    gat[0, pl.ds(96, 8), :] = groups[0] + groups[1] + groups[2]
    row8 = lax.broadcasted_iota(jnp.int32, (8, LANES), 0)
    folded = jnp.where(row8 < 3, groups[3], 0.0)
    for i in (1, 2):
        third = jnp.where((row8 >= 3 * i) & (row8 < 3 * i + 3), groups[3], 0.0)
        folded = folded + pltpu.roll(pltpu.roll(third, 8 - 3 * i, 0), REST * i, 1)
    gat[0, pl.ds(104, 8), :] = folded

    pl.semaphore_wait(barrier, 7)
    forward_after(0, far=False)
    for where in beside[:6]:
        pl.semaphore_signal(ready_sem, inc=1, device_id=where, device_id_type=MESH)
    for slot, offset in offsets.items():
        z, x, y = (
            lax.rem(pos + n - o, n) for pos, o, n in zip(me, offset, TORUS)
        )
        srow[slot] = ((z * TORUS[1] + x) * TORUS[2] + y) * own * 8

    acc[...] = jnp.zeros(acc.shape, F32)
    for c in range(2):
        tail_rows = kraw.shape[1] - rows_k
        kraw[c, pl.ds(rows_k, tail_rows), :] = jnp.zeros((tail_rows, LANES), F32)
    loads[3].wait()
    loads[4].wait()
    loads[5].wait()
    loads[6].wait()

    def transpose_tile(ft):
        parity, half = divmod(ft, 2)
        base = (2 * half * LANES + parity) * 8

        @pl.loop(0, 8)
        def _(i):
            st = i // 4
            p = lax.rem(i, 4)
            for c in range(2):
                block = kraw[c, pl.ds(base + st * 4 + p, LANES, stride=16), :]
                turned = block.T
                if c == 1 and ft == 0:
                    first = lax.broadcasted_iota(jnp.int32, (LANES, LANES), 1) == 0
                    turned = jnp.where(first, 0.0, turned)
                kt[ft, pl.ds(st * LANES * 8 + c * 4 + p, LANES, stride=8), :] = turned


    def consume(first, count):
        number = 32 * count
        for j in range(count):
            tile2 = gat[first + j, pl.ds(64, 32), :]
            left = gat[first + j, pl.ds(96, 16), :]
            moved2 = pltpu.roll(tile2, PIECE, 1)
            for g in range(4):
                if g < 3:
                    back = pltpu.roll(left[0:8], (PIECE - REST * g) % LANES, 1)
                else:
                    thirds = [
                        pltpu.roll(left[8:16], (PIECE - REST * i) % LANES, 1) for i in range(3)
                    ]
                    back = jnp.where(
                        row8 < 3,
                        thirds[0],
                        jnp.where(row8 < 6, pltpu.roll(thirds[1], 3, 0), pltpu.roll(thirds[2], 6, 0)),
                    )
                value = jnp.where(
                    lane8 < PIECE,
                    moved2[8 * g : 8 * g + 8],
                    jnp.where(lane8 < PIECE + REST, back, 0.0),
                )
                eb[pl.ds(32 * j + 8 * g, 8), :] = value

        def tiles(row):
            return gat[pl.ds(first, count), pl.ds(row, 32), :].reshape(number, LANES)

        even_re = jnp.concatenate([tiles(0), tiles(64)], axis=1)
        do[pl.ds(0, number), pl.ds(256, 256)] = times(even_re, ah[0], al[0])
        even_im = jnp.concatenate([tiles(32), eb[pl.ds(0, number), :]], axis=1)
        do[pl.ds(0, number), pl.ds(0, 256)] = times(even_im, ah[1], al[1])

        def d_value(ft, j, s, h, imag):
            inner = s * 16 + h * 8
            if ft == 0:
                return gat[first + j, pl.ds((32 if imag else 0) + inner, 8), :]
            if ft == 1:
                if imag:
                    return eb[pl.ds(pl.multiple_of(j * 32 + inner, 8), 8), :]
                return gat[first + j, pl.ds(64 + inner, 8), :]
            return do[
                pl.ds(pl.multiple_of(j * 32 + inner, 8), 8),
                pl.ds((256 if imag else 0) + (ft - 2) * LANES, LANES),
            ]

        for ft in range(4):
            start = tuple(
                acc[c, pl.ds(p * 16 + h * 8, 8), pl.ds(ft * LANES, LANES)]
                for c in range(2)
                for p in range(4)
                for h in range(2)
            )

            def sensors(j, sums):
                sums = list(sums)
                row = srow[first + j]
                for s in range(own):
                    d_re = [d_value(ft, j, s, h, False) for h in range(2)]
                    d_im = [d_value(ft, j, s, h, True) for h in range(2)]
                    for p in range(4):
                        at = pl.multiple_of(row + s * 8, 8)
                        k_re = jnp.broadcast_to(kt[ft, pl.ds(at + p, 1), :], (8, LANES))
                        k_im = jnp.broadcast_to(kt[ft, pl.ds(at + 4 + p, 1), :], (8, LANES))
                        for h in range(2):
                            i = p * 2 + h
                            sums[i] = sums[i] + k_re * d_re[h] + k_im * d_im[h]
                            sums[8 + i] = sums[8 + i] + k_re * d_im[h] - k_im * d_re[h]
                return tuple(sums)

            final = lax.fori_loop(0, count, sensors, start, unroll=True)
            for i, value in enumerate(final):
                c, p, h = i // 8, i // 2 % 4, i % 2
                acc[c, pl.ds(p * 16 + h * 8, 8), pl.ds(ft * LANES, LANES)] = value

    transpose_tile(0)
    pl.semaphore_wait(ready_sem, 6)
    forward_after(0, near=False)
    transpose_tile(1)

    @pl.loop(1, last)
    def _(k):
        copy(0, GROUP * k - 5, GROUP, k - 1, beside[0]).wait_recv()
        forward_between(k, 1, last)

        @pl.when(k == 1)
        def _():
            transpose_tile(2)
            transpose_tile(3)

        @pl.when(k == 2)
        def _():
            consume(0, 1)

        low = jnp.where(k == 2, 0, k - 1)
        high = jnp.where(k == 1, 0, k)

        @pl.loop(low, high)
        def _(b):
            consume(1 + GROUP * b, GROUP)

    copy(0, GROUP * (last - 1) + 1, rest_of, last - 1, beside[0]).wait_recv()
    consume(GROUP * (last - 1) + 1, rest_of)

    out_re = acc[0] * gain[0:1, :]
    out_im = acc[1] * gain[1:2, :]
    s_re = out_re[:, 0:256] + times(out_im[:, 256:512], ah[0], al[0], True)
    s_im = out_im[:, 0:256] + times(out_re[:, 256:512], ah[1], al[1], True)
    total = times(s_re, fh[:, 0:256], fl[:, 0:256], True) + times(
        s_im, fh[:, 256:512], fl[:, 256:512], True
    )
    part[...] = total
    swap = pltpu.make_async_remote_copy(
        src_ref=part,
        dst_ref=other,
        send_sem=pair_sem.at[0],
        recv_sem=pair_sem.at[1],
        device_id=partner,
        device_id_type=MESH,
    )
    swap.start()
    copy(1, 1, gat.shape[0] - 1, 0, beside[0]).wait_send()
    swap.wait()
    field = part[...] + other[...]
    square = field * field
    square = square[:, 0:128] + square[:, 128:256] + square[:, 256:384] + square[:, 384:512]
    square = square[0:16] + square[16:32] + square[32:48] + square[48:64]
    diagonal = lax.broadcasted_iota(jnp.int32, (16, LANES), 0) == lax.broadcasted_iota(
        jnp.int32, (16, LANES), 1
    )
    z, x, y = me
    spot = x * TORUS[2] + y

    def message(ref, mine, count, first, where):
        part_of = ref.at[pl.ds(mine, count)]
        return pltpu.make_async_remote_copy(
            src_ref=part_of,
            dst_ref=part_of,
            send_sem=red_sem.at[first],
            recv_sem=red_sem.at[first + 1],
            device_id=where,
            device_id_type=MESH,
        )

    def total_of(ref):
        total = ref[0]
        for i in range(1, ref.shape[0]):
            total = total + ref[i]
        return total

    @pl.when(core == 1)
    def _():
        column = jnp.sum(square, axis=1, keepdims=True)
        red1[spot] = jnp.sum(jnp.where(diagonal, column, 0.0), axis=0, keepdims=True)
        peers = [(0, dx, dy) for dx in range(TORUS[1]) for dy in range(TORUS[2]) if dx + dy > 0]
        for offset in peers:
            message(red1, spot, 1, 0, device(offset)).start()
        message(red1, 0, len(peers), 0, beside[0]).wait()
        red2[z] = total_of(red1)
        line = [(dz, 0, 0) for dz in range(TORUS[0])]
        for offset in line[1:]:
            message(red2, z, 1, 2, device(offset)).start()
        for offset in line:
            message(red2, z, 1, 2, dict(device(offset), sensor=0)).start()
        message(red2, 0, TORUS[0] - 1, 2, beside[0]).wait_recv()
        message(red1, 0, 2 * TORUS[0] - 1, 2, beside[0]).wait_send()

    @pl.when(core == 0)
    def _():
        message(red2, 0, TORUS[0], 2, beside[0]).wait_recv()

    whole = total_of(red2)
    count = 4 * math.prod(TORUS) * length
    rms = jnp.sqrt(whole / count + 1e-6)
    rms_ref[...] = rms[0, 0:16]
    column = jnp.sum(jnp.where(diagonal, 1.0 / rms, 0.0), axis=1, keepdims=True)
    for p in range(4):
        field_ref[:, p, :] = field[16 * p : 16 * p + 16, 0:length] * column


def body(data, spectra):
    vectors, own, length = data.shape
    freqs = length + 1
    sensors = spectra.shape[1]
    points = spectra.shape[2]
    forward, across, gains = spectral_tables(length)
    fh, fl = high_low(forward)
    ah, al = high_low(across)
    k_rows = jnp.transpose(
        spectra.reshape(2, sensors // LANES, LANES, points, freqs), (0, 4, 1, 3, 2)
    ).reshape(2, freqs * 8, LANES)
    devices = math.prod(TORUS)
    vmem = pltpu.VMEM
    field, rms = pl.pallas_call(
        kernel,
        out_shape=(
            pltpu.VMEM((vectors, points, length), F32),
            pltpu.VMEM((vectors,), F32),
        ),
        in_specs=[pl.BlockSpec(memory_space=pltpu.HBM)] * 7,
        out_specs=[pl.BlockSpec(memory_space=pltpu.VMEM)] * 2,
        scratch_shapes=[
            vmem((devices, ROWS, LANES), F32),
            vmem((vectors, own, length), F32),
            vmem((vectors * own, 512), F32),
            vmem((2, 4096, LANES), F32),
            vmem((4, sensors * 8, LANES), F32),
            vmem((512, 512), BF16),
            vmem((512, 512), BF16),
            vmem((2, 256, 256), BF16),
            vmem((2, 256, 256), BF16),
            vmem((8, 512), F32),
            vmem((192, LANES), F32),
            vmem((192, 512), F32),
            vmem((2, points * vectors, 512), F32),
            vmem((points * vectors, 512), F32),
            vmem((points * vectors, 512), F32),
            vmem((16, 1, LANES), F32),
            vmem((8, 1, LANES), F32),
            pltpu.SMEM((devices,), jnp.int32),
            pltpu.SemaphoreType.DMA,
            pltpu.SemaphoreType.DMA(((len(COPIES) - 1) // GROUP + 1,)),
            pltpu.SemaphoreType.DMA((7,)),
            pltpu.SemaphoreType.DMA((2,)),
            pltpu.SemaphoreType.DMA((4,)),
            pltpu.SemaphoreType.REGULAR,
        ],
        compiler_params=pltpu.CompilerParams(
            collective_id=0, has_side_effects=True, vmem_limit_bytes=VMEM_LIMIT
        ),
        name="adjoint",
    )(data, k_rows, jnp.asarray(fh), jnp.asarray(fl), jnp.asarray(ah), jnp.asarray(al), jnp.asarray(gains, F32))
    return (field, rms)


def solution(mesh):
    split_mesh = Mesh(
        mesh.devices.reshape(*TORUS, mesh.shape["sensor"]), (*PARAM, "sensor")
    )
    placed = (P(None, SENSOR_PARAM, None), P(None, "sensor", PARAM, None))
    return jax.shard_map(
        body, mesh=split_mesh, in_specs=placed, out_specs=(P(None, PARAM, None), P()), check_vma=False
    )
```

```python
import functools
import math

import jax
import jax.numpy as jnp
import numpy as np
from jax import lax
from jax.experimental import pallas as pl
from jax.experimental.pallas import tpu as pltpu
from jax.sharding import Mesh
from jax.sharding import PartitionSpec as P

PARAM = ("param_0", "param_1", "param_2")
SENSOR_PARAM = ("sensor", "param_0", "param_1", "param_2")
MESH = pl.DeviceIdType.MESH
F32 = jnp.float32
BF16 = jnp.bfloat16
TORUS = (8, 4, 4)
VECTORS = (
    (0, 1, 0),
    (0, -1, 0),
    (0, 0, 1),
    (0, 0, -1),
    (1, 0, 0),
    (-1, 0, 0),
    (-1, -1, 0),
    (-1, 0, -1),
    (0, -1, -1),
    (0, 1, -1),
    (0, 1, 1),
    (1, -1, 0),
    (1, 0, 1),
    (2, 0, 0),
)
COPIES = (
    (0, 0, 0, 3), (0, 0, 1, 4), (0, 0, 2, 1), (0, 0, 3, 2), (0, 0, 4, 5),
    (0, 0, 5, 6), (0, 0, 6, 7), (0, 0, 11, 11), (0, 0, 12, 10), (0, 0, 10, 8),
    (0, 0, 9, 9), (0, 0, 7, 12), (0, 0, 8, 17), (1, 4, 2, 13), (1, 5, 4, 15),
    (1, 5, 0, 14), (1, 6, 5, 16), (1, 5, 3, 19), (1, 4, 1, 18), (1, 6, 2, 20),
    (1, 6, 0, 21), (2, 7, 7, 25), (2, 11, 13, 31), (2, 7, 1, 24), (2, 8, 2, 22),
    (2, 10, 0, 23), (2, 12, 0, 30), (2, 11, 1, 27), (2, 12, 5, 28), (2, 12, 3, 29),
    (2, 10, 2, 26), (3, 14, 4, 35), (3, 17, 3, 33), (3, 16, 5, 36), (3, 15, 2, 34),
    (3, 17, 1, 32), (3, 16, 0, 37), (3, 15, 3, 39), (3, 15, 4, 41), (3, 16, 2, 42),
    (3, 7, 5, 43), (3, 8, 0, 38), (3, 15, 1, 40), (4, 24, 3, 49), (4, 23, 4, 46),
    (4, 24, 2, 48), (4, 22, 5, 47), (4, 19, 1, 45), (4, 23, 0, 44), (5, 27, 4, 52),
    (5, 25, 3, 55), (5, 25, 1, 54), (5, 26, 0, 50), (5, 11, 2, 51), (5, 25, 5, 53),
    (6, 31, 3, 58), (6, 36, 5, 59), (6, 31, 2, 57), (6, 31, 4, 60), (6, 36, 0, 61),
    (6, 31, 1, 56), (7, 37, 2, 66), (7, 29, 1, 67), (7, 35, 3, 63), (7, 32, 4, 62),
    (7, 41, 0, 64), (7, 42, 5, 65), (8, 47, 5, 72), (8, 46, 4, 70), (8, 42, 1, 73),
    (8, 46, 2, 68), (8, 46, 0, 69), (8, 36, 3, 71), (9, 53, 3, 78), (9, 50, 0, 74),
    (9, 48, 2, 79), (9, 53, 1, 77), (9, 39, 4, 75), (9, 53, 5, 76), (10, 59, 0, 82),
    (10, 48, 5, 85), (10, 60, 2, 84), (10, 56, 3, 81), (10, 56, 4, 83), (10, 57, 1, 80),
    (11, 58, 3, 87), (11, 66, 5, 89), (11, 55, 1, 91), (11, 61, 0, 90), (11, 62, 4, 86),
    (11, 65, 2, 88), (12, 68, 4, 93), (12, 59, 2, 94), (12, 61, 3, 96), (12, 68, 0, 92),
    (12, 65, 1, 97), (12, 72, 5, 95), (13, 34, 2, 98), (13, 76, 0, 99), (13, 70, 4, 100),
    (13, 78, 5, 102), (13, 77, 3, 103), (13, 76, 1, 101), (14, 83, 2, 109), (14, 75, 0, 107),
    (14, 57, 5, 105), (14, 26, 1, 104), (14, 34, 4, 106), (14, 81, 3, 108), (15, 82, 3, 113),
    (15, 45, 4, 110), (15, 88, 5, 112), (15, 90, 2, 114), (15, 36, 1, 115), (15, 87, 0, 111),
    (16, 42, 2, 119), (16, 85, 3, 121), (16, 92, 0, 117), (16, 95, 5, 118), (16, 96, 4, 120),
    (16, 33, 1, 116), (17, 9, 4, 123), (17, 102, 1, 124), (17, 7, 3, 127), (17, 20, 0, 125),
    (17, 13, 5, 126), (17, 1, 2, 122),
)
ROWS = 112
SENT = 107
GROUP = 6
LANES = 128
PIECE = 45
REST = 37
VMEM_LIMIT = 66_000_000


def moved(offset, step):
    return tuple((a + b) % n for a, b, n in zip(offset, step, TORUS))


def hops(offset):
    return sum(min(o, n - o) for o, n in zip(offset, TORUS))


def spectral_tables(steps):
    half = steps // 2
    t = np.arange(steps)[:, None]
    even = 2 * np.arange(half + 1)[None, :]
    odd = 2 * np.arange(half)[None, :] + 1
    turn = math.pi / steps
    even_re = np.cos(turn * (t * even % (2 * steps)))
    even_im = -np.sin(turn * (t * even % (2 * steps)))
    even_im[:, 0] = np.arange(steps) == 0
    even_im[:, half] = 0.0
    odd_re = np.cos(turn * (t * odd % (2 * steps)))
    odd_im = -np.sin(turn * (t * odd % (2 * steps)))
    forward = np.zeros((512, 512))
    forward[:steps, : half + 1] = even_re
    forward[:steps, 256 : 256 + half + 1] = even_im
    weight = np.full((half + 1,), 2.0 / steps)
    weight[0] = weight[half] = 1.0 / steps
    across = np.zeros((2, 256, 256))
    across[0, : half + 1, :half] = weight[:, None] * (even_re.T @ odd_im)
    across[1, : half + 1, :half] = weight[:, None] * (even_im.T @ odd_re)
    across[1, 0, :half] = 1.0
    gains = np.zeros((8, 512))
    gains[0, : half + 1] = weight / 2
    gains[0, 256 : 256 + half] = 1.0 / steps
    gains[1] = gains[0]
    gains[1, 0] = 0.0
    return (forward, across, gains)


def high_low(array):
    array = array.astype(np.float32)
    high = array.astype(jnp.bfloat16)
    low = (array - high.astype(np.float32)).astype(jnp.bfloat16)
    return (high, low)


def split(value):
    high = value.astype(BF16)
    return (high, (value - high.astype(F32)).astype(BF16))


def times(value, high, low, transposed=False):
    dims = (((1,), (1 if transposed else 0,)), ((), ()))
    dot = functools.partial(lax.dot_general, dimension_numbers=dims, preferred_element_type=F32)
    upper, lower = split(value)
    return dot(upper, high) + dot(lower, high) + dot(upper, low)


def kernel(
    data_ref,
    k_ref,
    fh_ref,
    fl_ref,
    ah_ref,
    al_ref,
    gain_ref,
    field_ref,
    rms_ref,
    gat,
    xv,
    xs,
    kraw,
    kt,
    fh,
    fl,
    ah,
    al,
    gain,
    eb,
    do,
    acc,
    part,
    other,
    red1,
    red2,
    srow,
    send_sem,
    recv_sem,
    load_sem,
    pair_sem,
    red_sem,
    ready_sem,
):
    vectors, own, length = data_ref.shape
    me = tuple(lax.axis_index(name) for name in PARAM)
    core = lax.axis_index("sensor")

    def device(offset):
        return {
            name: lax.rem(pos + (o % n), n) for name, pos, o, n in zip(PARAM, me, offset, TORUS)
        }

    beside = [device(offset) for offset in VECTORS]
    partner = {"sensor": 1 - core}
    barrier = pltpu.get_barrier_semaphore()
    for where in beside[:6]:
        pl.semaphore_signal(barrier, inc=1, device_id=where, device_id_type=MESH)
    pl.semaphore_signal(barrier, inc=1, device_id=partner, device_id_type=MESH)

    rows_k = k_ref.shape[1]
    loads = [
        pltpu.make_async_copy(data_ref, xv, load_sem.at[0]),
        pltpu.make_async_copy(fh_ref, fh, load_sem.at[1]),
        pltpu.make_async_copy(fl_ref, fl, load_sem.at[2]),
        pltpu.make_async_copy(k_ref, kraw.at[:, pl.ds(0, rows_k), :], load_sem.at[3]),
        pltpu.make_async_copy(ah_ref, ah, load_sem.at[4]),
        pltpu.make_async_copy(al_ref, al, load_sem.at[5]),
        pltpu.make_async_copy(gain_ref, gain, load_sem.at[6]),
    ]
    for load in loads:
        load.start()

    offsets = {0: (0, 0, 0)}
    for _, source, vector, target in COPIES:
        offsets[target] = moved(offsets[source], VECTORS[vector])
    last = (len(COPIES) - 1) // GROUP + 1
    rest_of = len(COPIES) - GROUP * (last - 1)

    def copy(source, target, count, step, where):
        return pltpu.make_async_remote_copy(
            src_ref=gat.at[pl.ds(source, count), pl.ds(0, SENT)],
            dst_ref=gat.at[pl.ds(target, count), pl.ds(0, SENT)],
            send_sem=send_sem,
            recv_sem=recv_sem.at[step],
            device_id=where,
            device_id_type=MESH,
        )

    def forward_after(k, near=True, far=True):
        for when, source, vector, target in COPIES:
            if when == k and (near if vector < 6 else far):
                copy(source, target, 1, (target - 1) // GROUP, beside[vector]).start()

    def forward_between(k, low, high):
        if high - low == 1:
            forward_after(low)
        else:
            middle = (low + high) // 2
            lax.cond(
                k < middle,
                lambda: forward_between(k, low, middle),
                lambda: forward_between(k, middle, high),
            )

    xs[:, pl.ds(384, LANES)] = jnp.zeros((2 * vectors, LANES), F32)
    loads[0].wait()
    for r in range(vectors):
        for s in range(own):
            xs[pl.ds(s * vectors + r, 1), pl.ds(0, length)] = xv[r, pl.ds(s, 1), :]
    loads[1].wait()
    loads[2].wait()
    spec = times(xs[...], fh[...], fl[...])
    lane = lax.broadcasted_iota(jnp.int32, (32, LANES), 1)
    lane8 = lax.broadcasted_iota(jnp.int32, (8, LANES), 1)
    re_b = spec[:, 128:256]
    im_b = spec[:, 384:512]
    gat[0, pl.ds(0, 32), :] = spec[:, 0:128]
    gat[0, pl.ds(32, 32), :] = spec[:, 256:384]
    gat[0, pl.ds(64, 32), :] = re_b + pltpu.roll(
        jnp.where(lane < PIECE, im_b, 0.0), LANES - PIECE, 1
    )
    rest = jnp.where((lane >= PIECE) & (lane < PIECE + REST), im_b, 0.0)
    groups = [
        pltpu.roll(rest[8 * g : 8 * g + 8], (REST * (g % 3) - PIECE) % LANES, 1) for g in range(4)
    ]
    gat[0, pl.ds(96, 8), :] = groups[0] + groups[1] + groups[2]
    row8 = lax.broadcasted_iota(jnp.int32, (8, LANES), 0)
    folded = jnp.where(row8 < 3, groups[3], 0.0)
    for i in (1, 2):
        third = jnp.where((row8 >= 3 * i) & (row8 < 3 * i + 3), groups[3], 0.0)
        folded = folded + pltpu.roll(pltpu.roll(third, 8 - 3 * i, 0), REST * i, 1)
    gat[0, pl.ds(104, 8), :] = folded

    pl.semaphore_wait(barrier, 7)
    @pl.when(core == 0)
    def _():
        forward_after(0, far=False)

    for where in beside[:6]:
        pl.semaphore_signal(ready_sem, inc=1, device_id=where, device_id_type=MESH)
    for slot, offset in offsets.items():
        z, x, y = (
            lax.rem(pos + n - o, n) for pos, o, n in zip(me, offset, TORUS)
        )
        srow[slot] = ((z * TORUS[1] + x) * TORUS[2] + y) * own * 8

    acc[...] = jnp.zeros(acc.shape, F32)
    for c in range(2):
        tail_rows = kraw.shape[1] - rows_k
        kraw[c, pl.ds(rows_k, tail_rows), :] = jnp.zeros((tail_rows, LANES), F32)
    loads[3].wait()
    loads[4].wait()
    loads[5].wait()
    loads[6].wait()

    @pl.when(core == 1)
    def _():
        forward_after(0, far=False)

    def transpose_tile(ft):
        parity, half = divmod(ft, 2)
        base = (2 * half * LANES + parity) * 8

        @pl.loop(0, 8)
        def _(i):
            st = i // 4
            p = lax.rem(i, 4)
            for c in range(2):
                block = kraw[c, pl.ds(base + st * 4 + p, LANES, stride=16), :]
                turned = block.T
                if c == 1 and ft == 0:
                    first = lax.broadcasted_iota(jnp.int32, (LANES, LANES), 1) == 0
                    turned = jnp.where(first, 0.0, turned)
                kt[ft, pl.ds(st * LANES * 8 + c * 4 + p, LANES, stride=8), :] = turned


    def consume(first, count):
        number = 32 * count
        for j in range(count):
            tile2 = gat[first + j, pl.ds(64, 32), :]
            left = gat[first + j, pl.ds(96, 16), :]
            moved2 = pltpu.roll(tile2, PIECE, 1)
            for g in range(4):
                if g < 3:
                    back = pltpu.roll(left[0:8], (PIECE - REST * g) % LANES, 1)
                else:
                    thirds = [
                        pltpu.roll(left[8:16], (PIECE - REST * i) % LANES, 1) for i in range(3)
                    ]
                    back = jnp.where(
                        row8 < 3,
                        thirds[0],
                        jnp.where(row8 < 6, pltpu.roll(thirds[1], 3, 0), pltpu.roll(thirds[2], 6, 0)),
                    )
                value = jnp.where(
                    lane8 < PIECE,
                    moved2[8 * g : 8 * g + 8],
                    jnp.where(lane8 < PIECE + REST, back, 0.0),
                )
                eb[pl.ds(32 * j + 8 * g, 8), :] = value

        def tiles(row):
            return gat[pl.ds(first, count), pl.ds(row, 32), :].reshape(number, LANES)

        even_re = jnp.concatenate([tiles(0), tiles(64)], axis=1)
        do[pl.ds(0, number), pl.ds(256, 256)] = times(even_re, ah[0], al[0])
        even_im = jnp.concatenate([tiles(32), eb[pl.ds(0, number), :]], axis=1)
        do[pl.ds(0, number), pl.ds(0, 256)] = times(even_im, ah[1], al[1])

        def d_value(ft, j, s, h, imag):
            inner = s * 16 + h * 8
            if ft == 0:
                return gat[first + j, pl.ds((32 if imag else 0) + inner, 8), :]
            if ft == 1:
                if imag:
                    return eb[pl.ds(pl.multiple_of(j * 32 + inner, 8), 8), :]
                return gat[first + j, pl.ds(64 + inner, 8), :]
            return do[
                pl.ds(pl.multiple_of(j * 32 + inner, 8), 8),
                pl.ds((256 if imag else 0) + (ft - 2) * LANES, LANES),
            ]

        for ft in range(4):
            start = tuple(
                acc[c, pl.ds(p * 16 + h * 8, 8), pl.ds(ft * LANES, LANES)]
                for c in range(2)
                for p in range(4)
                for h in range(2)
            )

            def sensors(j, sums):
                sums = list(sums)
                row = srow[first + j]
                for s in range(own):
                    d_re = [d_value(ft, j, s, h, False) for h in range(2)]
                    d_im = [d_value(ft, j, s, h, True) for h in range(2)]
                    for p in range(4):
                        at = pl.multiple_of(row + s * 8, 8)
                        k_re = jnp.broadcast_to(kt[ft, pl.ds(at + p, 1), :], (8, LANES))
                        k_im = jnp.broadcast_to(kt[ft, pl.ds(at + 4 + p, 1), :], (8, LANES))
                        for h in range(2):
                            i = p * 2 + h
                            sums[i] = sums[i] + k_re * d_re[h] + k_im * d_im[h]
                            sums[8 + i] = sums[8 + i] + k_re * d_im[h] - k_im * d_re[h]
                return tuple(sums)

            final = lax.fori_loop(0, count, sensors, start, unroll=True)
            for i, value in enumerate(final):
                c, p, h = i // 8, i // 2 % 4, i % 2
                acc[c, pl.ds(p * 16 + h * 8, 8), pl.ds(ft * LANES, LANES)] = value

    transpose_tile(0)
    pl.semaphore_wait(ready_sem, 6)
    forward_after(0, near=False)
    transpose_tile(1)

    @pl.loop(1, last)
    def _(k):
        copy(0, GROUP * k - 5, GROUP, k - 1, beside[0]).wait_recv()
        forward_between(k, 1, last)

        @pl.when(k == 1)
        def _():
            transpose_tile(2)
            transpose_tile(3)

        @pl.when(k == 2)
        def _():
            consume(0, 2)

        low = jnp.maximum(k - 2, 0)
        high = jnp.maximum(k - 1, 0)

        @pl.loop(low, high)
        def _(b):
            consume(2 + GROUP * b, GROUP)

    copy(0, GROUP * (last - 1) + 1, rest_of, last - 1, beside[0]).wait_recv()
    consume(GROUP * (last - 2) + 2, GROUP)

    out_re = acc[0] * gain[0:1, :]
    out_im = acc[1] * gain[1:2, :]
    s_re = out_re[:, 0:256] + times(out_im[:, 256:512], ah[0], al[0], True)
    s_im = out_im[:, 0:256] + times(out_re[:, 256:512], ah[1], al[1], True)
    total = times(s_re, fh[:, 0:256], fl[:, 0:256], True) + times(
        s_im, fh[:, 256:512], fl[:, 256:512], True
    )
    part[...] = total
    swap = pltpu.make_async_remote_copy(
        src_ref=part,
        dst_ref=other,
        send_sem=pair_sem.at[0],
        recv_sem=pair_sem.at[1],
        device_id=partner,
        device_id_type=MESH,
    )
    swap.start()
    copy(1, 1, gat.shape[0] - 1, 0, beside[0]).wait_send()
    swap.wait()
    field = part[...] + other[...]
    square = field * field
    square = square[:, 0:128] + square[:, 128:256] + square[:, 256:384] + square[:, 384:512]
    square = square[0:16] + square[16:32] + square[32:48] + square[48:64]
    diagonal = lax.broadcasted_iota(jnp.int32, (16, LANES), 0) == lax.broadcasted_iota(
        jnp.int32, (16, LANES), 1
    )
    z, x, y = me
    spot = x * TORUS[2] + y

    def message(ref, mine, count, first, where):
        part_of = ref.at[pl.ds(mine, count)]
        return pltpu.make_async_remote_copy(
            src_ref=part_of,
            dst_ref=part_of,
            send_sem=red_sem.at[first],
            recv_sem=red_sem.at[first + 1],
            device_id=where,
            device_id_type=MESH,
        )

    def total_of(ref):
        total = ref[0]
        for i in range(1, ref.shape[0]):
            total = total + ref[i]
        return total

    @pl.when(core == 1)
    def _():
        column = jnp.sum(square, axis=1, keepdims=True)
        red1[spot] = jnp.sum(jnp.where(diagonal, column, 0.0), axis=0, keepdims=True)
        peers = [(0, dx, dy) for dx in range(TORUS[1]) for dy in range(TORUS[2]) if dx + dy > 0]
        peers.sort(key=hops, reverse=True)
        for offset in peers:
            message(red1, spot, 1, 0, device(offset)).start()
        message(red1, 0, len(peers), 0, beside[0]).wait()
        red2[z] = total_of(red1)
        line = [(dz, 0, 0) for dz in range(TORUS[0])]
        line.sort(key=hops, reverse=True)
        for offset in line:
            message(red2, z, 1, 2, dict(device(offset), sensor=0)).start()
            if hops(offset) > 0:
                message(red2, z, 1, 2, device(offset)).start()
        message(red2, 0, TORUS[0] - 1, 2, beside[0]).wait_recv()
        message(red1, 0, 2 * TORUS[0] - 1, 2, beside[0]).wait_send()

    @pl.when(core == 0)
    def _():
        message(red2, 0, TORUS[0], 2, beside[0]).wait_recv()

    whole = total_of(red2)
    count = 4 * math.prod(TORUS) * length
    rms = jnp.sqrt(whole / count + 1e-6)
    rms_ref[...] = rms[0, 0:16]
    column = jnp.sum(jnp.where(diagonal, 1.0 / rms, 0.0), axis=1, keepdims=True)
    for p in range(4):
        field_ref[:, p, :] = field[16 * p : 16 * p + 16, 0:length] * column


def body(data, spectra):
    vectors, own, length = data.shape
    freqs = length + 1
    sensors = spectra.shape[1]
    points = spectra.shape[2]
    forward, across, gains = spectral_tables(length)
    fh, fl = high_low(forward)
    ah, al = high_low(across)
    k_rows = jnp.transpose(
        spectra.reshape(2, sensors // LANES, LANES, points, freqs), (0, 4, 1, 3, 2)
    ).reshape(2, freqs * 8, LANES)
    devices = math.prod(TORUS)
    vmem = pltpu.VMEM
    field, rms = pl.pallas_call(
        kernel,
        out_shape=(
            pltpu.VMEM((vectors, points, length), F32),
            pltpu.VMEM((vectors,), F32),
        ),
        in_specs=[pl.BlockSpec(memory_space=pltpu.HBM)] * 7,
        out_specs=[pl.BlockSpec(memory_space=pltpu.VMEM)] * 2,
        scratch_shapes=[
            vmem((devices, ROWS, LANES), F32),
            vmem((vectors, own, length), F32),
            vmem((vectors * own, 512), F32),
            vmem((2, 4096, LANES), F32),
            vmem((4, sensors * 8, LANES), F32),
            vmem((512, 512), BF16),
            vmem((512, 512), BF16),
            vmem((2, 256, 256), BF16),
            vmem((2, 256, 256), BF16),
            vmem((8, 512), F32),
            vmem((192, LANES), F32),
            vmem((192, 512), F32),
            vmem((2, points * vectors, 512), F32),
            vmem((points * vectors, 512), F32),
            vmem((points * vectors, 512), F32),
            vmem((16, 1, LANES), F32),
            vmem((8, 1, LANES), F32),
            pltpu.SMEM((devices,), jnp.int32),
            pltpu.SemaphoreType.DMA,
            pltpu.SemaphoreType.DMA(((len(COPIES) - 1) // GROUP + 1,)),
            pltpu.SemaphoreType.DMA((7,)),
            pltpu.SemaphoreType.DMA((2,)),
            pltpu.SemaphoreType.DMA((4,)),
            pltpu.SemaphoreType.REGULAR,
        ],
        compiler_params=pltpu.CompilerParams(
            collective_id=0, has_side_effects=True, vmem_limit_bytes=VMEM_LIMIT
        ),
        name="adjoint",
    )(data, k_rows, jnp.asarray(fh), jnp.asarray(fl), jnp.asarray(ah), jnp.asarray(al), jnp.asarray(gains, F32))
    return (field, rms)


def solution(mesh):
    split_mesh = Mesh(
        mesh.devices.reshape(*TORUS, mesh.shape["sensor"]), (*PARAM, "sensor")
    )
    placed = (P(None, SENSOR_PARAM, None), P(None, "sensor", PARAM, None))
    return jax.shard_map(
        body, mesh=split_mesh, in_specs=placed, out_specs=(P(None, PARAM, None), P()), check_vma=False
    )
```

```python
import functools
import math

import jax
import jax.numpy as jnp
import numpy as np
from jax import lax
from jax.experimental import pallas as pl
from jax.experimental.pallas import tpu as pltpu
from jax.sharding import Mesh
from jax.sharding import PartitionSpec as P

PARAM = ("param_0", "param_1", "param_2")
SENSOR_PARAM = ("sensor", "param_0", "param_1", "param_2")
MESH = pl.DeviceIdType.MESH
F32 = jnp.float32
BF16 = jnp.bfloat16
TORUS = (8, 4, 4)
VECTORS = (
    (0, 1, 0),
    (0, -1, 0),
    (0, 0, 1),
    (0, 0, -1),
    (1, 0, 0),
    (-1, 0, 0),
    (-1, -1, 0),
    (-1, 0, -1),
    (0, -1, -1),
    (0, 1, -1),
    (0, 1, 1),
    (1, -1, 0),
    (1, 0, 1),
    (2, 0, 0),
)
COPIES = (
    (0, 0, 0, 3), (0, 0, 1, 4), (0, 0, 2, 1), (0, 0, 3, 2), (0, 0, 4, 5),
    (0, 0, 5, 6), (0, 0, 6, 7), (0, 0, 11, 11), (0, 0, 12, 10), (0, 0, 10, 8),
    (0, 0, 9, 9), (0, 0, 7, 12), (0, 0, 8, 17), (1, 4, 2, 13), (1, 5, 4, 15),
    (1, 5, 0, 14), (1, 6, 5, 16), (1, 5, 3, 19), (1, 4, 1, 18), (1, 6, 2, 20),
    (1, 6, 0, 21), (2, 7, 7, 25), (2, 11, 13, 31), (2, 7, 1, 24), (2, 8, 2, 22),
    (2, 10, 0, 23), (2, 12, 0, 30), (2, 11, 1, 27), (2, 12, 5, 28), (2, 12, 3, 29),
    (2, 10, 2, 26), (3, 14, 4, 35), (3, 17, 3, 33), (3, 16, 5, 36), (3, 15, 2, 34),
    (3, 17, 1, 32), (3, 16, 0, 37), (3, 15, 3, 39), (3, 15, 4, 41), (3, 16, 2, 42),
    (3, 7, 5, 43), (3, 8, 0, 38), (3, 15, 1, 40), (4, 24, 3, 49), (4, 23, 4, 46),
    (4, 24, 2, 48), (4, 22, 5, 47), (4, 19, 1, 45), (4, 23, 0, 44), (5, 27, 4, 52),
    (5, 25, 3, 55), (5, 25, 1, 54), (5, 26, 0, 50), (5, 11, 2, 51), (5, 25, 5, 53),
    (6, 31, 3, 58), (6, 36, 5, 59), (6, 31, 2, 57), (6, 31, 4, 60), (6, 36, 0, 61),
    (6, 31, 1, 56), (7, 37, 2, 66), (7, 29, 1, 67), (7, 35, 3, 63), (7, 32, 4, 62),
    (7, 41, 0, 64), (7, 42, 5, 65), (8, 47, 5, 72), (8, 46, 4, 70), (8, 42, 1, 73),
    (8, 46, 2, 68), (8, 46, 0, 69), (8, 36, 3, 71), (9, 53, 3, 78), (9, 50, 0, 74),
    (9, 48, 2, 79), (9, 53, 1, 77), (9, 39, 4, 75), (9, 53, 5, 76), (10, 59, 0, 82),
    (10, 48, 5, 85), (10, 60, 2, 84), (10, 56, 3, 81), (10, 56, 4, 83), (10, 57, 1, 80),
    (11, 58, 3, 87), (11, 66, 5, 89), (11, 55, 1, 91), (11, 61, 0, 90), (11, 62, 4, 86),
    (11, 65, 2, 88), (12, 68, 4, 93), (12, 59, 2, 94), (12, 61, 3, 96), (12, 68, 0, 92),
    (12, 65, 1, 97), (12, 72, 5, 95), (13, 34, 2, 98), (13, 76, 0, 99), (13, 70, 4, 100),
    (13, 78, 5, 102), (13, 77, 3, 103), (13, 76, 1, 101), (14, 83, 2, 109), (14, 75, 0, 107),
    (14, 57, 5, 105), (14, 26, 1, 104), (14, 34, 4, 106), (14, 81, 3, 108), (15, 82, 3, 113),
    (15, 45, 4, 110), (15, 88, 5, 112), (15, 90, 2, 114), (15, 36, 1, 115), (15, 87, 0, 111),
    (16, 42, 2, 119), (16, 85, 3, 121), (16, 92, 0, 117), (16, 95, 5, 118), (16, 96, 4, 120),
    (16, 33, 1, 116), (17, 9, 4, 123), (17, 102, 1, 124), (17, 7, 3, 127), (17, 20, 0, 125),
    (17, 13, 5, 126), (17, 1, 2, 122),
)
ROWS = 112
SENT = 107
GROUP = 6
LANES = 128
PIECE = 45
REST = 37
VMEM_LIMIT = 66_000_000


def moved(offset, step):
    return tuple((a + b) % n for a, b, n in zip(offset, step, TORUS))


def hops(offset):
    return sum(min(o, n - o) for o, n in zip(offset, TORUS))


def spectral_tables(steps):
    half = steps // 2
    t = np.arange(steps)[:, None]
    even = 2 * np.arange(half + 1)[None, :]
    odd = 2 * np.arange(half)[None, :] + 1
    turn = math.pi / steps
    even_re = np.cos(turn * (t * even % (2 * steps)))
    even_im = -np.sin(turn * (t * even % (2 * steps)))
    even_im[:, 0] = np.arange(steps) == 0
    even_im[:, half] = 0.0
    odd_re = np.cos(turn * (t * odd % (2 * steps)))
    odd_im = -np.sin(turn * (t * odd % (2 * steps)))
    forward = np.zeros((512, 512))
    forward[:steps, : half + 1] = even_re
    forward[:steps, 256 : 256 + half + 1] = even_im
    weight = np.full((half + 1,), 2.0 / steps)
    weight[0] = weight[half] = 1.0 / steps
    across = np.zeros((2, 256, 256))
    across[0, : half + 1, :half] = weight[:, None] * (even_re.T @ odd_im)
    across[1, : half + 1, :half] = weight[:, None] * (even_im.T @ odd_re)
    across[1, 0, :half] = 1.0
    gains = np.zeros((8, 512))
    gains[0, : half + 1] = weight / 2
    gains[0, 256 : 256 + half] = 1.0 / steps
    gains[1] = gains[0]
    gains[1, 0] = 0.0
    return (forward, across, gains)


def high_low(array):
    array = array.astype(np.float32)
    high = array.astype(jnp.bfloat16)
    low = (array - high.astype(np.float32)).astype(jnp.bfloat16)
    return (high, low)


def split(value):
    high = value.astype(BF16)
    return (high, (value - high.astype(F32)).astype(BF16))


def times(value, high, low, transposed=False):
    dims = (((1,), (1 if transposed else 0,)), ((), ()))
    dot = functools.partial(lax.dot_general, dimension_numbers=dims, preferred_element_type=F32)
    upper, lower = split(value)
    return dot(upper, high) + dot(lower, high) + dot(upper, low)


def kernel(
    data_ref,
    k_ref,
    fh_ref,
    fl_ref,
    ah_ref,
    al_ref,
    gain_ref,
    field_ref,
    rms_ref,
    gat,
    xv,
    xs,
    kraw,
    kt,
    fh,
    fl,
    ah,
    al,
    gain,
    eb,
    do,
    acc,
    part,
    other,
    red1,
    red2,
    srow,
    send_sem,
    recv_sem,
    load_sem,
    pair_sem,
    red_sem,
    ready_sem,
):
    vectors, own, length = data_ref.shape
    me = tuple(lax.axis_index(name) for name in PARAM)
    core = lax.axis_index("sensor")

    def device(offset):
        return {
            name: lax.rem(pos + (o % n), n) for name, pos, o, n in zip(PARAM, me, offset, TORUS)
        }

    beside = [device(offset) for offset in VECTORS]
    partner = {"sensor": 1 - core}
    barrier = pltpu.get_barrier_semaphore()
    for where in beside[:6]:
        pl.semaphore_signal(barrier, inc=1, device_id=where, device_id_type=MESH)
    pl.semaphore_signal(barrier, inc=1, device_id=partner, device_id_type=MESH)

    rows_k = k_ref.shape[1]
    loads = [
        pltpu.make_async_copy(data_ref, xv, load_sem.at[0]),
        pltpu.make_async_copy(fh_ref, fh, load_sem.at[1]),
        pltpu.make_async_copy(fl_ref, fl, load_sem.at[2]),
        pltpu.make_async_copy(k_ref, kraw.at[:, pl.ds(0, rows_k), :], load_sem.at[3]),
        pltpu.make_async_copy(ah_ref, ah, load_sem.at[4]),
        pltpu.make_async_copy(al_ref, al, load_sem.at[5]),
        pltpu.make_async_copy(gain_ref, gain, load_sem.at[6]),
    ]
    for load in loads:
        load.start()

    offsets = {0: (0, 0, 0)}
    for _, source, vector, target in COPIES:
        offsets[target] = moved(offsets[source], VECTORS[vector])
    last = (len(COPIES) - 1) // GROUP + 1
    rest_of = len(COPIES) - GROUP * (last - 1)

    def copy(source, target, count, step, where):
        return pltpu.make_async_remote_copy(
            src_ref=gat.at[pl.ds(source, count), pl.ds(0, SENT)],
            dst_ref=gat.at[pl.ds(target, count), pl.ds(0, SENT)],
            send_sem=send_sem,
            recv_sem=recv_sem.at[step],
            device_id=where,
            device_id_type=MESH,
        )

    def forward_after(k, near=True, far=True):
        for when, source, vector, target in COPIES:
            if when == k and (near if vector < 6 else far):
                copy(source, target, 1, (target - 1) // GROUP, beside[vector]).start()

    def forward_between(k, low, high):
        if high - low == 1:
            forward_after(low)
        else:
            middle = (low + high) // 2
            lax.cond(
                k < middle,
                lambda: forward_between(k, low, middle),
                lambda: forward_between(k, middle, high),
            )

    xs[:, pl.ds(384, LANES)] = jnp.zeros((2 * vectors, LANES), F32)
    loads[0].wait()
    for r in range(vectors):
        for s in range(own):
            xs[pl.ds(s * vectors + r, 1), pl.ds(0, length)] = xv[r, pl.ds(s, 1), :]
    loads[1].wait()
    loads[2].wait()
    spec = times(xs[...], fh[...], fl[...])
    lane = lax.broadcasted_iota(jnp.int32, (32, LANES), 1)
    lane8 = lax.broadcasted_iota(jnp.int32, (8, LANES), 1)
    re_b = spec[:, 128:256]
    im_b = spec[:, 384:512]
    gat[0, pl.ds(0, 32), :] = spec[:, 0:128]
    gat[0, pl.ds(32, 32), :] = spec[:, 256:384]
    gat[0, pl.ds(64, 32), :] = re_b + pltpu.roll(
        jnp.where(lane < PIECE, im_b, 0.0), LANES - PIECE, 1
    )
    rest = jnp.where((lane >= PIECE) & (lane < PIECE + REST), im_b, 0.0)
    groups = [
        pltpu.roll(rest[8 * g : 8 * g + 8], (REST * (g % 3) - PIECE) % LANES, 1) for g in range(4)
    ]
    gat[0, pl.ds(96, 8), :] = groups[0] + groups[1] + groups[2]
    row8 = lax.broadcasted_iota(jnp.int32, (8, LANES), 0)
    folded = jnp.where(row8 < 3, groups[3], 0.0)
    for i in (1, 2):
        third = jnp.where((row8 >= 3 * i) & (row8 < 3 * i + 3), groups[3], 0.0)
        folded = folded + pltpu.roll(pltpu.roll(third, 8 - 3 * i, 0), REST * i, 1)
    gat[0, pl.ds(104, 8), :] = folded

    pl.semaphore_wait(barrier, 7)
    @pl.when(core == 0)
    def _():
        forward_after(0, far=False)

    for where in beside[:6]:
        pl.semaphore_signal(ready_sem, inc=1, device_id=where, device_id_type=MESH)
    for slot, offset in offsets.items():
        z, x, y = (
            lax.rem(pos + n - o, n) for pos, o, n in zip(me, offset, TORUS)
        )
        srow[slot] = ((z * TORUS[1] + x) * TORUS[2] + y) * own * 8

    acc[...] = jnp.zeros(acc.shape, F32)
    for c in range(2):
        tail_rows = kraw.shape[1] - rows_k
        kraw[c, pl.ds(rows_k, tail_rows), :] = jnp.zeros((tail_rows, LANES), F32)
    loads[3].wait()
    loads[4].wait()
    loads[5].wait()
    loads[6].wait()

    @pl.when(core == 1)
    def _():
        forward_after(0, far=False)

    def transpose_tile(ft):
        parity, half = divmod(ft, 2)
        base = (2 * half * LANES + parity) * 8

        @pl.loop(0, 8)
        def _(i):
            st = i // 4
            p = lax.rem(i, 4)
            for c in range(2):
                block = kraw[c, pl.ds(base + st * 4 + p, LANES, stride=16), :]
                turned = block.T
                if c == 1 and ft == 0:
                    first = lax.broadcasted_iota(jnp.int32, (LANES, LANES), 1) == 0
                    turned = jnp.where(first, 0.0, turned)
                kt[ft, pl.ds(st * LANES * 8 + c * 4 + p, LANES, stride=8), :] = turned


    def consume(first, count):
        number = 32 * count
        for j in range(count):
            tile2 = gat[first + j, pl.ds(64, 32), :]
            left = gat[first + j, pl.ds(96, 16), :]
            moved2 = pltpu.roll(tile2, PIECE, 1)
            for g in range(4):
                if g < 3:
                    back = pltpu.roll(left[0:8], (PIECE - REST * g) % LANES, 1)
                else:
                    thirds = [
                        pltpu.roll(left[8:16], (PIECE - REST * i) % LANES, 1) for i in range(3)
                    ]
                    back = jnp.where(
                        row8 < 3,
                        thirds[0],
                        jnp.where(row8 < 6, pltpu.roll(thirds[1], 3, 0), pltpu.roll(thirds[2], 6, 0)),
                    )
                value = jnp.where(
                    lane8 < PIECE,
                    moved2[8 * g : 8 * g + 8],
                    jnp.where(lane8 < PIECE + REST, back, 0.0),
                )
                eb[pl.ds(32 * j + 8 * g, 8), :] = value

        def tiles(row):
            return gat[pl.ds(first, count), pl.ds(row, 32), :].reshape(number, LANES)

        even_re = jnp.concatenate([tiles(0), tiles(64)], axis=1)
        do[pl.ds(0, number), pl.ds(256, 256)] = times(even_re, ah[0], al[0])
        even_im = jnp.concatenate([tiles(32), eb[pl.ds(0, number), :]], axis=1)
        do[pl.ds(0, number), pl.ds(0, 256)] = times(even_im, ah[1], al[1])

        def d_value(ft, j, s, h, imag):
            inner = s * 16 + h * 8
            if ft == 0:
                return gat[first + j, pl.ds((32 if imag else 0) + inner, 8), :]
            if ft == 1:
                if imag:
                    return eb[pl.ds(pl.multiple_of(j * 32 + inner, 8), 8), :]
                return gat[first + j, pl.ds(64 + inner, 8), :]
            return do[
                pl.ds(pl.multiple_of(j * 32 + inner, 8), 8),
                pl.ds((256 if imag else 0) + (ft - 2) * LANES, LANES),
            ]

        for ft in range(4):
            start = tuple(
                acc[c, pl.ds(p * 16 + h * 8, 8), pl.ds(ft * LANES, LANES)]
                for c in range(2)
                for p in range(4)
                for h in range(2)
            )

            def sensors(j, sums):
                sums = list(sums)
                row = srow[first + j]
                for s in range(own):
                    d_re = [d_value(ft, j, s, h, False) for h in range(2)]
                    d_im = [d_value(ft, j, s, h, True) for h in range(2)]
                    for p in range(4):
                        at = pl.multiple_of(row + s * 8, 8)
                        k_re = jnp.broadcast_to(kt[ft, pl.ds(at + p, 1), :], (8, LANES))
                        k_im = jnp.broadcast_to(kt[ft, pl.ds(at + 4 + p, 1), :], (8, LANES))
                        for h in range(2):
                            i = p * 2 + h
                            sums[i] = sums[i] + k_re * d_re[h] + k_im * d_im[h]
                            sums[8 + i] = sums[8 + i] + k_re * d_im[h] - k_im * d_re[h]
                return tuple(sums)

            final = lax.fori_loop(0, count, sensors, start, unroll=True)
            for i, value in enumerate(final):
                c, p, h = i // 8, i // 2 % 4, i % 2
                acc[c, pl.ds(p * 16 + h * 8, 8), pl.ds(ft * LANES, LANES)] = value

    transpose_tile(0)
    pl.semaphore_wait(ready_sem, 6)
    forward_after(0, near=False)
    transpose_tile(1)

    @pl.loop(1, last)
    def _(k):
        copy(0, GROUP * k - 5, GROUP, k - 1, beside[0]).wait_recv()
        forward_between(k, 1, last)

        @pl.when(k == 1)
        def _():
            transpose_tile(2)

        @pl.when(k == 2)
        def _():
            transpose_tile(3)
            consume(0, 2)

        low = jnp.maximum(k - 2, 0)
        high = jnp.maximum(k - 1, 0)

        @pl.loop(low, high)
        def _(b):
            consume(2 + GROUP * b, GROUP)

    copy(0, GROUP * (last - 1) + 1, rest_of, last - 1, beside[0]).wait_recv()
    consume(GROUP * (last - 2) + 2, GROUP)

    out_re = acc[0] * gain[0:1, :]
    out_im = acc[1] * gain[1:2, :]
    s_re = out_re[:, 0:256] + times(out_im[:, 256:512], ah[0], al[0], True)
    s_im = out_im[:, 0:256] + times(out_re[:, 256:512], ah[1], al[1], True)
    total = times(s_re, fh[:, 0:256], fl[:, 0:256], True) + times(
        s_im, fh[:, 256:512], fl[:, 256:512], True
    )
    part[...] = total
    swap = pltpu.make_async_remote_copy(
        src_ref=part,
        dst_ref=other,
        send_sem=pair_sem.at[0],
        recv_sem=pair_sem.at[1],
        device_id=partner,
        device_id_type=MESH,
    )
    swap.start()
    copy(1, 1, gat.shape[0] - 1, 0, beside[0]).wait_send()
    swap.wait()
    field = part[...] + other[...]
    square = field * field
    square = square[:, 0:128] + square[:, 128:256] + square[:, 256:384] + square[:, 384:512]
    square = square[0:16] + square[16:32] + square[32:48] + square[48:64]
    diagonal = lax.broadcasted_iota(jnp.int32, (16, LANES), 0) == lax.broadcasted_iota(
        jnp.int32, (16, LANES), 1
    )
    z, x, y = me
    spot = x * TORUS[2] + y

    def message(ref, mine, count, first, where):
        part_of = ref.at[pl.ds(mine, count)]
        return pltpu.make_async_remote_copy(
            src_ref=part_of,
            dst_ref=part_of,
            send_sem=red_sem.at[first],
            recv_sem=red_sem.at[first + 1],
            device_id=where,
            device_id_type=MESH,
        )

    def total_of(ref):
        total = ref[0]
        for i in range(1, ref.shape[0]):
            total = total + ref[i]
        return total

    @pl.when(core == 1)
    def _():
        column = jnp.sum(square, axis=1, keepdims=True)
        red1[spot] = jnp.sum(jnp.where(diagonal, column, 0.0), axis=0, keepdims=True)
        peers = [(0, dx, dy) for dx in range(TORUS[1]) for dy in range(TORUS[2]) if dx + dy > 0]
        peers.sort(key=hops, reverse=True)
        for offset in peers:
            message(red1, spot, 1, 0, device(offset)).start()
        message(red1, 0, len(peers), 0, beside[0]).wait()
        red2[z] = total_of(red1)
        line = [(dz, 0, 0) for dz in range(TORUS[0])]
        line.sort(key=hops, reverse=True)
        for offset in line:
            message(red2, z, 1, 2, dict(device(offset), sensor=0)).start()
            if hops(offset) > 0:
                message(red2, z, 1, 2, device(offset)).start()
        message(red2, 0, TORUS[0] - 1, 2, beside[0]).wait_recv()
        message(red1, 0, 2 * TORUS[0] - 1, 2, beside[0]).wait_send()

    @pl.when(core == 0)
    def _():
        message(red2, 0, TORUS[0], 2, beside[0]).wait_recv()

    whole = total_of(red2)
    count = 4 * math.prod(TORUS) * length
    rms = jnp.sqrt(whole / count + 1e-6)
    rms_ref[...] = rms[0, 0:16]
    column = jnp.sum(jnp.where(diagonal, 1.0 / rms, 0.0), axis=1, keepdims=True)
    for p in range(4):
        field_ref[:, p, :] = field[16 * p : 16 * p + 16, 0:length] * column


def body(data, spectra):
    vectors, own, length = data.shape
    freqs = length + 1
    sensors = spectra.shape[1]
    points = spectra.shape[2]
    forward, across, gains = spectral_tables(length)
    fh, fl = high_low(forward)
    ah, al = high_low(across)
    k_rows = jnp.transpose(
        spectra.reshape(2, sensors // LANES, LANES, points, freqs), (0, 4, 1, 3, 2)
    ).reshape(2, freqs * 8, LANES)
    devices = math.prod(TORUS)
    vmem = pltpu.VMEM
    field, rms = pl.pallas_call(
        kernel,
        out_shape=(
            pltpu.VMEM((vectors, points, length), F32),
            pltpu.VMEM((vectors,), F32),
        ),
        in_specs=[pl.BlockSpec(memory_space=pltpu.HBM)] * 7,
        out_specs=[pl.BlockSpec(memory_space=pltpu.VMEM)] * 2,
        scratch_shapes=[
            vmem((devices, ROWS, LANES), F32),
            vmem((vectors, own, length), F32),
            vmem((vectors * own, 512), F32),
            vmem((2, 4096, LANES), F32),
            vmem((4, sensors * 8, LANES), F32),
            vmem((512, 512), BF16),
            vmem((512, 512), BF16),
            vmem((2, 256, 256), BF16),
            vmem((2, 256, 256), BF16),
            vmem((8, 512), F32),
            vmem((192, LANES), F32),
            vmem((192, 512), F32),
            vmem((2, points * vectors, 512), F32),
            vmem((points * vectors, 512), F32),
            vmem((points * vectors, 512), F32),
            vmem((16, 1, LANES), F32),
            vmem((8, 1, LANES), F32),
            pltpu.SMEM((devices,), jnp.int32),
            pltpu.SemaphoreType.DMA,
            pltpu.SemaphoreType.DMA(((len(COPIES) - 1) // GROUP + 1,)),
            pltpu.SemaphoreType.DMA((7,)),
            pltpu.SemaphoreType.DMA((2,)),
            pltpu.SemaphoreType.DMA((4,)),
            pltpu.SemaphoreType.REGULAR,
        ],
        compiler_params=pltpu.CompilerParams(
            collective_id=0, has_side_effects=True, vmem_limit_bytes=VMEM_LIMIT
        ),
        name="adjoint",
    )(data, k_rows, jnp.asarray(fh), jnp.asarray(fl), jnp.asarray(ah), jnp.asarray(al), jnp.asarray(gains, F32))
    return (field, rms)


def solution(mesh):
    split_mesh = Mesh(
        mesh.devices.reshape(*TORUS, mesh.shape["sensor"]), (*PARAM, "sensor")
    )
    placed = (P(None, SENSOR_PARAM, None), P(None, "sensor", PARAM, None))
    return jax.shard_map(
        body, mesh=split_mesh, in_specs=placed, out_specs=(P(None, PARAM, None), P()), check_vma=False
    )
```
